32 devices in a mesh: grp: 2 (over x), slab: 16 (over z, y, core).
Axes of the slice: x: 2, y: 2, z: 4, core: 2. Of those that a mesh axis runs over, the one named last changes fastest.
Arguments:
- volume: bfloat16 [64, 1024, 1024], P(('grp', 'slab')), parts along dimension 0, may hold values from -60 to 60
- plane_shift: int32 [4, 32], P('grp', 'slab'), parts along dimension 0, may hold values from -64 to 64
- plane_weight: float32 [4, 32], P('grp', 'slab'), parts along dimension 0, may hold values from 0 to 1
- column_left: int32 [4, 1024], P('grp'), parts along dimension 0, may hold values from 0 to 1022
- column_weight: float32 [4, 1024], P('grp'), parts along dimension 0, may hold values from 0 to 1
- window_center: int32 [4, 2], P('grp'), parts along dimension 0, may hold values from -200 to 199
- tilt_owner: int32 [32], P('grp'), parts along dimension 0, may hold values from 0 to 15, each once
- reference_band: float32 [32, 2, 128, 128], P(('grp', 'slab')), parts along dimension 0, may hold values from -6 to 6
Outputs:
- correlation: float32 [4, 16, 128], P('grp', 'slab'), parts along dimension 0
- peaks: float32 [4], P('grp'), parts along dimension 0
The draws below stay inside these ranges and needn't reach their ends.
There are 2 independent parts, one for each index of `grp`. The reference program is written for one: setup_inputs(seed, part) draws one part's arguments, and reference() takes and returns one part's arrays. A program takes and returns all parts, laid end to end along the dimension named above; each array names one. Nothing has to cross between parts.
Inputs may be any that keep to these rules, and one draw needn't show every extreme that they name: `tilt_owner`: the first 2 entries name the owners of the tilts, one slab index each.
All inputs are finite; a program needn't handle non-finite values.
Results may differ from the reference program's by a relative error of at most 0.0003.
Values sent between devices are 32-bit elements; how exact they have to be, the bound alone decides.
A program may use at most 128 MiB of HBM per device.

```python
import math
import jax
import jax.numpy as jnp
from jax import lax

Y = 1024
X = 1024
BAND = 128
WIN_COLS = 128
TILTS = 2
PLANES = 32
WIN_ROWS = 16
N_SLAB = 16


def draw_volume(key, part):
    first_key, second_key, third_key = jax.random.split(key, 3)
    col_scale = jnp.exp(jax.random.uniform(second_key, (1, 1, X), jnp.float32) * math.log(10.0))
    row_scale = jnp.exp(jax.random.uniform(third_key, (1, Y, 1), jnp.float32) * math.log(10.0))
    base = jnp.clip(jax.random.normal(first_key, (PLANES, Y, X), jnp.float32), -6.0, 6.0)
    return (base * col_scale * row_scale / 10.0).astype(jnp.bfloat16)


def set_ends(values, own_key, smallest, high):
    dims = values.shape
    place = [jax.random.randint(jax.random.fold_in(own_key, axis), (), 0, dims[axis]) for axis in range(len(dims))]
    values = values.at[tuple(place)].set(smallest)
    longest = dims.index(max(dims))
    place[longest] = (place[longest] + 1) % dims[longest]
    return values.at[tuple(place)].set(high)


def level_of(key, extent, pieces, least, largest):
    factor_of = 1.0
    for dim, shards_of in pieces:
        draws = jax.random.uniform(jax.random.fold_in(jax.random.fold_in(key, 6), dim), (shards_of,), jnp.float32, least / len(pieces), largest / len(pieces))
        factor_of = factor_of * jnp.repeat(jnp.exp(draws), extent[dim] // shards_of).reshape((-1,) + (1,) * (len(extent) - 1 - dim))
    return factor_of


def gaussian(own_key, extent, spread, most, cuts=(), kind=jnp.bfloat16):
    result = jax.random.normal(own_key, extent, jnp.float32) * spread
    if len(cuts) > 0:
        result = level_of(own_key, extent, cuts, -0.22, 0.18) * result
    return jnp.clip(result, min=-most, max=most).astype(kind)


def setup_inputs(seed: int = 0, part: int = 0) -> dict:
    seeds = jax.random.split(jax.random.key(seed), 9)
    own_keys = jax.random.split(jax.random.fold_in(seeds[8], part), 9)
    volume = draw_volume(jax.random.fold_in(jax.random.fold_in(seeds[8], part), 71), part)
    plane_shift = set_ends(jax.random.randint(own_keys[1], (TILTS, PLANES), -(X // 16), X // 16 + 1), jax.random.fold_in(own_keys[1], 1), -(X // 16), (X // 16 + 1) - 1).astype(jnp.int32)
    plane_weight = jnp.clip(1.0 * jax.random.uniform(own_keys[2], (TILTS, PLANES), jnp.float32) ** level_of(own_keys[2], (TILTS, PLANES), ((1, 16),), -0.2, 0.2), 0.0, 1.0)
    column_left = set_ends(jax.random.randint(own_keys[3], (TILTS, X), 0, X - 1), jax.random.fold_in(own_keys[3], 1), 0, (X - 1) - 1).astype(jnp.int32)
    column_weight = jnp.clip(jax.random.uniform(own_keys[4], (TILTS, X), jnp.float32, 0.0, 1.0), 0.0, 1.0)
    window_center = set_ends(jax.random.randint(own_keys[5], (TILTS, 2), -200, 200), jax.random.fold_in(own_keys[5], 1), -200, 199).astype(jnp.int32)
    tilt_owner = jax.random.permutation(own_keys[6], N_SLAB).astype(jnp.int32)
    reference_band = gaussian(own_keys[7], (N_SLAB, 2, BAND, BAND), 1.0, 6.0, ((0, 16),), jnp.float32)
    return {"volume": volume, "plane_shift": plane_shift, "plane_weight": plane_weight, "column_left": column_left, "column_weight": column_weight, "window_center": window_center, "tilt_owner": tilt_owner, "reference_band": reference_band}


def project_tilt(volume, shift_row, weight_row, left_row, share_row):
    margin = X // 16 + 1

    def add_plane(total, items):
        plane_data, shift_value, weight_value = items
        padded = jnp.pad(plane_data.astype(jnp.float32), ((0, 0), (margin, margin)))
        near_cells = lax.dynamic_slice_in_dim(padded, (margin - shift_value).astype(jnp.int32), X, 1)
        far_cells = lax.dynamic_slice_in_dim(padded, (margin - shift_value - 1).astype(jnp.int32), X, 1)
        return (total + (1.0 - weight_value) * near_cells + weight_value * far_cells, None)
    summed, _ = lax.scan(add_plane, jnp.zeros((Y, X), jnp.float32), (volume, shift_row, weight_row))
    left_values = jnp.take(summed, left_row, axis=1)
    right_values = jnp.take(summed, left_row + 1, axis=1)
    return (1.0 - share_row) * left_values + share_row * right_values

def phase_pair(left_ints, right_ints, length):
    product = left_ints[:, None] * right_ints[None, :] % length
    angle = product.astype(jnp.float32) * (2.0 * math.pi / length)
    return (jnp.cos(angle), jnp.sin(angle))

def matmul(first, second):
    return jnp.dot(first, second, precision=lax.Precision.HIGHEST, preferred_element_type=jnp.float32)

def reference(volume, plane_shift, plane_weight, column_left, column_weight, window_center, tilt_owner, reference_band):
    freq_cols = jnp.arange(BAND, dtype=jnp.int32)
    freq_rows = freq_cols - BAND // 2
    band_rows = freq_rows % Y
    outputs = []
    maxima = []
    for which in range(TILTS):
        projected = project_tilt(volume, plane_shift[which], plane_weight[which], column_left[which], column_weight[which])
        full_spec = jnp.fft.fft2(projected)
        band_spec = jnp.take(full_spec, band_rows, axis=0)[:, :BAND]
        spec_real = jnp.real(band_spec).astype(jnp.float32)
        spec_imag = jnp.imag(band_spec).astype(jnp.float32)
        owned = reference_band[tilt_owner[which]]
        ref_real, ref_imag = (owned[0], owned[1])
        cross_real = spec_real * ref_real + spec_imag * ref_imag
        cross_imag = spec_imag * ref_real - spec_real * ref_imag
        energy_spec = jnp.mean(spec_real * spec_real + spec_imag * spec_imag) + 1e-06
        energy_ref = jnp.mean(ref_real * ref_real + ref_imag * ref_imag) + 1e-06
        offsets_y = window_center[which, 0] + jnp.arange(WIN_ROWS, dtype=jnp.int32) - WIN_ROWS // 2
        offsets_x = window_center[which, 1] + jnp.arange(WIN_COLS, dtype=jnp.int32) - WIN_COLS // 2
        row_cos, row_sin = phase_pair(offsets_y, freq_rows, Y)
        col_cos, col_sin = phase_pair(freq_cols, offsets_x, X)
        half_real = matmul(row_cos, cross_real) - matmul(row_sin, cross_imag)
        half_imag = matmul(row_cos, cross_imag) + matmul(row_sin, cross_real)
        corr = (matmul(half_real, col_cos) - matmul(half_imag, col_sin)) / (BAND * jnp.sqrt(energy_spec * energy_ref))
        outputs.append(corr)
        maxima.append(jnp.max(corr))
    return (jnp.stack(outputs), jnp.stack(maxima))
```

```python
import functools
import math

import jax
import jax.numpy as jnp
import numpy as np
from jax import lax
from jax.experimental import pallas as pl
from jax.experimental.pallas import tpu as pltpu
from jax.sharding import PartitionSpec as P

MESH = pl.DeviceIdType.MESH
LANES = 128
SUBLANES = 8
CHUNK = 256
OWNERS = 4
BF16 = jnp.bfloat16
F32 = jnp.float32


def phases(left, right, length):
    angle = (np.outer(left, right) % length) * (2.0 * math.pi / length)
    return np.cos(angle), np.sin(angle)


def split(values):
    high = values.astype(np.float32).astype(BF16)
    low = (values - high.astype(np.float64)).astype(np.float32).astype(BF16)
    return high, low


def halves(value):
    high = value.astype(BF16)
    return high, (value - high.astype(F32)).astype(BF16)


def row_table(length, band):
    half = band // 2
    cos, sin = phases(np.arange(half + 1), np.arange(length), length)
    last = np.zeros((SUBLANES, length))
    last[0] = sin[half]
    return np.concatenate(split(np.concatenate([cos[:half], cos[half:], sin[1:half], last])))


def col_table(length, band, owners):
    cos, sin = phases(np.arange(band), np.arange(length), length)
    own = band // owners
    rows = []
    for w in range(owners):
        rows += [cos[w * own : (w + 1) * own], sin[w * own : (w + 1) * own]]
    return np.concatenate(split(np.concatenate(rows)))


def fused_kernel(
    n, owners, center_hbm, owner_hbm, shift_hbm, weight_hbm,
    left_ref, share_ref, mine_ref, volume_ref, rowt_ref, colt_ref, corr_ref, peak_ref,
    center_ref, owner_ref, shift_ref, weight_ref, left, share, mine, vol, rowt, colt, onehot, shares, rows, extra, line, summed, stack, proj,
    perm, ref_out, ref_in, spec_out, spec_sib, spec_in, part_out, part_in,
    sems, ref_send, ref_recv, sib_send, sib_recv, spec_send, spec_recv, part_send, part_recv,
):
    me = lax.axis_index("slab")
    core = lax.rem(me, 2)
    sibling = me + 1 - 2 * core
    chip = me // 2
    planes, height, width = volume_ref.shape
    tilts = left_ref.shape[0]
    band = mine_ref.shape[-1]
    half = band // 2
    own = band // owners
    blocks = width // LANES
    chunks = width // CHUNK
    count = rowt_ref.shape[0] // 2
    pad = (rows.shape[1] - width) // 2
    length = width
    win_cols = corr_ref.shape[-1]
    first, stride = n // owners + 1, max(2, n // (2 * owners))
    places = [first + w * stride for w in range(owners)]

    def local(source, into, k):
        copy = pltpu.make_async_copy(source, into, sems.at[k])
        copy.start()
        return copy

    get_left = local(left_ref, left, 0)
    get_share = local(share_ref, share, 1)
    scalars = [
        local(shift_hbm, shift_ref, 2), local(weight_hbm, weight_ref, 3),
        local(center_hbm, center_ref, 4), local(owner_hbm, owner_ref, 5),
    ]
    get_table = local(rowt_ref, rowt, 6)
    get_mine = local(mine_ref, mine, 7)
    for z in range(planes):
        for c in range(chunks):
            part = (z, pl.ds(c * (height // chunks), height // chunks))
            local(volume_ref.at[part], vol.at[part], 9 + z)
    get_colt = local(colt_ref, colt, 8)

    barrier = pltpu.get_barrier_semaphore()
    for k in range(1, n):
        pl.semaphore_signal(
            barrier, inc=1, device_id={"slab": lax.rem(me + k, n)}, device_id_type=MESH
        )

    def remote(source, into, send, recv, device):
        return pltpu.make_async_remote_copy(
            src_ref=source, dst_ref=into, send_sem=send, recv_sem=recv,
            device_id={"slab": device}, device_id_type=MESH,
        )

    for z in range(planes):
        rows[z, :pad, :] = jnp.zeros((pad, LANES), F32)
        rows[z, pad + width :, :] = jnp.zeros((pad, LANES), F32)
    summed[width:, :] = jnp.zeros((SUBLANES, LANES), F32)
    line[...] = jnp.zeros(line.shape, F32)

    lane = lax.broadcasted_iota(jnp.int32, (LANES, LANES), 1)
    get_left.wait()
    get_share.wait()

    @pl.loop(0, blocks)
    def _(b):
        begin = pl.multiple_of(b * LANES, LANES)
        for t in range(tilts):
            row = left[t : t + 1, pl.ds(begin, LANES)].astype(F32)
            column = jnp.broadcast_to(row, (LANES, LANES)).T.astype(jnp.int32)
            for x in range(blocks):
                hit = jnp.where(column == lane + x * LANES, 1.0, 0.0)
                onehot[t, pl.ds(begin, LANES), x * LANES : (x + 1) * LANES] = hit.astype(BF16)
            row = share[t : t + 1, pl.ds(begin, LANES)]
            shares[t, pl.ds(begin, LANES), :] = jnp.broadcast_to(row, (LANES, LANES)).T

    get_mine.wait()
    for part in range(2):
        perm[:half, :] = mine[0, part, half:, :]
        for k in range(half):
            row = half - k if k else 0
            perm[half + k : half + k + 1, :] = mine[0, part, row : row + 1, :]
        turned = perm[...].T
        for w in range(owners):
            ref_out[w, part * own : (part + 1) * own, :] = turned[w * own : (w + 1) * own]

    get_table.wait()
    for z in range(planes):
        pltpu.make_async_copy(volume_ref.at[z], vol.at[z], sems.at[9 + z]).wait()
        for c in range(chunks):
            out = jnp.dot(
                rowt[...], vol[z, :, c * CHUNK : (c + 1) * CHUNK], preferred_element_type=F32
            )
            out = out[:count] + out[count:]
            for b in range(CHUNK // LANES):
                here = slice(b * LANES, (b + 1) * LANES)
                begin = c * CHUNK + b * LANES
                rows[z, pad + begin : pad + begin + LANES, :] = out[:band, here].T
                extra[z, begin // LANES : begin // LANES + 1, :] = out[band : band + 1, here]

    for copy in scalars:
        copy.wait()
    for t in range(tilts):
        base = jnp.concatenate(
            [left[t : t + 1, b * LANES : (b + 1) * LANES] for b in range(blocks)], axis=0
        )
        right = jnp.concatenate(
            [share[t : t + 1, b * LANES : (b + 1) * LANES] for b in range(blocks)], axis=0
        )
        value = None
        for z in range(planes):
            weight = weight_ref[t, z]
            taps = (
                (1, right * (1.0 - weight)),
                (0, (1.0 - right) * (1.0 - weight) + right * weight),
                (-1, (1.0 - right) * weight),
            )
            for step, factor in taps:
                index = base + (step - shift_ref[t, z])
                spot = index & (LANES - 1)
                block = lax.shift_right_arithmetic(index, int(math.log2(LANES)))
                found = jnp.zeros((blocks, LANES), F32)
                for b in range(blocks):
                    source = jnp.broadcast_to(extra[z, b : b + 1, :], (blocks, LANES))
                    source = jnp.take_along_axis(source, spot, axis=1)
                    found = jnp.where(block == b, source, found)
                value = factor * found if value is None else value + factor * found
        for b in range(blocks):
            line[t : t + 1, b * LANES : (b + 1) * LANES] = value[b : b + 1, :]

    def along(left_hand, right_hand, **kind):
        return lax.dot_general(
            left_hand, right_hand, (((1,), (1,)), ((), ())), preferred_element_type=F32, **kind
        )

    def prepare(t):
        for b in range(blocks):
            total = None
            for z in range(planes):
                weight = weight_ref[t, z]
                start = pad + b * LANES - shift_ref[t, z]
                near = rows[z, pl.ds(start, LANES), :]
                far = rows[z, pl.ds(start - 1, LANES), :]
                term = (1.0 - weight) * near + weight * far
                total = term if total is None else total + term
            here = slice(b * LANES, (b + 1) * LANES)
            summed[here, :] = total
            high, low = halves(total)
            stack[here, 0:LANES] = high
            stack[here, LANES : 2 * LANES] = low
        for b in range(blocks):
            here = slice(b * LANES, (b + 1) * LANES)
            high, low = halves(summed[b * LANES + 1 : (b + 1) * LANES + 1, :])
            stack[here, 2 * LANES : 3 * LANES] = high
            stack[here, 3 * LANES :] = low

    def gather(t):
        for c in range(chunks):
            here = slice(c * CHUNK, (c + 1) * CHUNK)
            picked = jnp.dot(onehot[t, here, :], stack[...], preferred_element_type=F32)
            near = picked[:, :LANES] + picked[:, LANES : 2 * LANES]
            far = picked[:, 2 * LANES : 3 * LANES] + picked[:, 3 * LANES :]
            part = shares[t, here, :]
            high, low = halves((1.0 - part) * near + part * far)
            proj[here, :LANES] = high
            proj[here, LANES:] = low

    def columns(t):
        both = jnp.dot(colt[...], proj[...], preferred_element_type=F32)
        top = 2 * band
        value = both[:top, :LANES] + both[:top, LANES:] + both[top:, :LANES]
        for w in range(owners):
            spec_out[t, w, : 2 * own, :] = value[w * 2 * own : (w + 1) * 2 * own]

    def to_sibling(t):
        return remote(spec_out.at[t], spec_sib.at[t], sib_send, sib_recv, sibling)

    def to_owner(t, w):
        return remote(
            spec_out.at[t, w], spec_in.at[t, chip], spec_send.at[w], spec_recv.at[t], places[w]
        )

    def to_others(make):
        for w in range(owners):
            pl.when(me != places[w])(lambda: make(w).start())

    def ref_to(w):
        return remote(ref_out.at[w], ref_in.at[me], ref_send.at[w], ref_recv, places[w])

    def pass_on(t):
        @pl.when(core == t % 2)
        def _():
            to_sibling(t).wait_recv()
            spec_out[t] = spec_out[t] + spec_sib[t]
            to_others(functools.partial(to_owner, t))

    for t in range(tilts):
        prepare(t)
        if t == 0:
            pl.semaphore_wait(barrier, n - 1)
            to_others(ref_to)
            get_colt.wait()
        gather(t)
        if t:
            pass_on(t - 1)
        else:
            value = line[...]
            high = value.astype(BF16).astype(F32)
            value = jnp.concatenate([high, value - high], axis=0).astype(BF16)
            one = along(value, colt[: 2 * band, :])
            two = along(value, colt[2 * band :, :])
            value = one[:SUBLANES] + one[SUBLANES:] + two[:SUBLANES]
            for w in range(owners):
                begin = w * 2 * own
                offset = begin % LANES
                block = value[:, begin - offset : begin - offset + LANES]
                if offset:
                    block = pltpu.roll(block, LANES - offset, 1)
                for s in range(tilts):
                    spec_out[s, w, 2 * own :, :] = block
        columns(t)

        @pl.when(core != t % 2)
        def _():
            to_sibling(t).start()

    pass_on(tilts - 1)

    def wave(ints):
        angle = (ints & (length - 1)).astype(F32) * (2.0 * math.pi / length)
        return jnp.cos(angle), jnp.sin(angle)

    is_owner = functools.reduce(jnp.logical_or, [me == place for place in places])
    slot = (me - first) // stride

    @pl.when(is_owner)
    def _():
        spot = lax.broadcasted_iota(jnp.int32, (n, band), 1)
        freq = jnp.where(spot < half, spot, jnp.where(spot == half, -half, half - spot))
        step = lax.broadcasted_iota(jnp.int32, (n, band), 0) - n // 2
        cols = lax.broadcasted_iota(jnp.int32, (own, win_cols), 0) + slot * own
        offset = lax.broadcasted_iota(jnp.int32, (own, win_cols), 1) - win_cols // 2
        row_waves, col_waves = [], []
        for t in range(tilts):
            row_waves.append(jnp.concatenate(wave(freq * (center_ref[t, 0] + step)), axis=0))
            cos, sin = wave(cols * (center_ref[t, 1] + offset))
            col_waves.append(jnp.concatenate([cos, -sin], axis=0))
        spot = lax.broadcasted_iota(jnp.int32, (own, band), 1)
        lower, start, middle = spot < half, spot == 0, spot == half
        ref_in[me] = ref_out[slot]
        remote(
            ref_in.at[pl.ds(0, n - 1)], ref_in.at[pl.ds(0, n - 1)], ref_send.at[0], ref_recv, me
        ).wait_recv()
        part_out[tilts * n :, :] = jnp.zeros((SUBLANES, win_cols), F32)
        for t in range(tilts):
            remote_count = n // 2
            if t % 2 == 1:
                spec_in[t, chip] = spec_out[t, slot]
                remote_count -= 1
            arrived = spec_in.at[t, pl.ds(0, remote_count)]
            remote(arrived, arrived, spec_send.at[0], spec_recv.at[t], me).wait_recv()
            total = spec_in[t, 0]
            for e in range(1, n // 2):
                total = total + spec_in[t, e]
            cos, sin = total[:own], total[own : 2 * own]
            last = total[2 * own :].T[:, t : t + 1]
            last_cos, last_sin = last[:own], last[own : 2 * own]
            cos_turn = pltpu.roll(cos, half, 1)
            sin_turn = pltpu.roll(sin, half, 1)
            spec_re = jnp.where(
                lower,
                cos - jnp.where(start, 0.0, sin_turn),
                jnp.where(middle, cos + last_sin, cos_turn + sin),
            )
            spec_im = jnp.where(
                lower,
                -(jnp.where(start, 0.0, cos_turn) + sin),
                jnp.where(middle, last_cos - sin, cos - sin_turn),
            )
            owned = ref_in[owner_ref[t]]
            ref_re, ref_im = owned[:own], owned[own:]
            cross_re = spec_re * ref_re + spec_im * ref_im
            cross_im = spec_im * ref_re - spec_re * ref_im
            for kind, (real, imag) in enumerate(((spec_re, spec_im), (ref_re, ref_im))):
                power = jnp.sum(real * real + imag * imag, axis=0, keepdims=True)
                row = tilts * n + kind * tilts + t
                part_out[row : row + 1, :] = power
            turned = along(
                row_waves[t], jnp.concatenate([cross_re, cross_im], axis=0),
                precision=lax.Precision.HIGHEST,
            )
            moved_re = turned[:n, :own] - turned[n:, own:]
            moved_im = turned[:n, own:] + turned[n:, :own]
            part_out[t * n : (t + 1) * n, :] = jnp.dot(
                jnp.concatenate([moved_re, moved_im], axis=1), col_waves[t],
                precision=lax.Precision.HIGHEST, preferred_element_type=F32,
            )
        for d in range(n):
            @pl.when(me != d)
            def _():
                remote(part_out, part_in.at[slot], part_send.at[d], part_recv.at[slot], d).start()
        part_in[slot] = part_out[...]

    for w in range(owners):
        @pl.when(me != places[w])
        def _():
            remote(part_in.at[w], part_in.at[w], part_send.at[0], part_recv.at[w], me).wait_recv()
    total = part_in[0]
    for w in range(1, owners):
        total = total + part_in[w]
    power = jnp.sum(total[tilts * n :], axis=1, keepdims=True) / (band * band) + 1e-06
    peaks = []
    mine_row = lax.broadcasted_iota(jnp.int32, (n, win_cols), 0) == me
    for t in range(tilts):
        scale = band * jnp.sqrt(power[t : t + 1] * power[tilts + t : tilts + t + 1])
        value = total[t * n : (t + 1) * n]
        row = jnp.sum(jnp.where(mine_row, value, 0.0), axis=0, keepdims=True)
        corr_ref[t] = row / scale
        peaks.append(jnp.max(jnp.max(value, axis=0, keepdims=True), axis=1, keepdims=True) / scale)

    spot = lax.broadcasted_iota(jnp.int32, (1, win_cols), 1)
    best = jnp.broadcast_to(peaks[0], (1, win_cols))
    for t in range(1, tilts):
        best = jnp.where(spot == t, peaks[t], best)
    peak_ref[...] = best[0, :tilts]

    def done(make):
        for w in range(owners):
            pl.when(me != places[w])(lambda: make(w).wait_send())

    done(ref_to)
    for t in range(tilts):
        @pl.when(core == t % 2)
        def _():
            done(functools.partial(to_owner, t))

        @pl.when(core != t % 2)
        def _():
            to_sibling(t).wait_send()

    @pl.when(is_owner)
    def _():
        for d in range(n):
            @pl.when(me != d)
            def _():
                remote(part_out, part_in.at[slot], part_send.at[d], part_recv.at[slot], d).wait_send()


def run(n, volume, shift, weight, left, share, center, owner, mine):
    planes, height, width = volume.shape
    tilts = left.shape[0]
    band = mine.shape[-1]
    win_cols = band
    owners = OWNERS
    rowt = row_table(height, band)
    colt = col_table(width, band, owners)
    blocks = width // LANES
    pad = width // 16 + SUBLANES
    own = band // owners
    message = (2 * own + SUBLANES, band)
    part = (tilts * n + SUBLANES, win_cols)
    smem = pl.BlockSpec(memory_space=pltpu.SMEM)
    vmem = pl.BlockSpec(memory_space=pltpu.VMEM)
    hbm = pl.BlockSpec(memory_space=pl.ANY)
    dma = pltpu.SemaphoreType.DMA
    return pl.pallas_call(
        functools.partial(fused_kernel, n, owners),
        out_shape=(
            pltpu.VMEM((tilts, 1, win_cols), F32),
            pltpu.VMEM((tilts,), F32),
        ),
        in_specs=[hbm] * 10,
        out_specs=(vmem, vmem),
        scratch_shapes=[
            pltpu.SMEM(center.shape, jnp.int32),
            pltpu.SMEM(owner.shape, jnp.int32),
            pltpu.SMEM(shift.shape, jnp.int32),
            pltpu.SMEM(weight.shape, F32),
            pltpu.VMEM(left.shape, jnp.int32),
            pltpu.VMEM(share.shape, F32),
            pltpu.VMEM(mine.shape, F32),
            pltpu.VMEM((planes, height, width), BF16),
            pltpu.VMEM(rowt.shape, BF16),
            pltpu.VMEM(colt.shape, BF16),
            pltpu.VMEM((tilts, width, width), BF16),
            pltpu.VMEM((tilts, width, LANES), F32),
            pltpu.VMEM((planes, width + 2 * pad, LANES), F32),
            pltpu.VMEM((planes, blocks, LANES), F32),
            pltpu.VMEM((SUBLANES, width), F32),
            pltpu.VMEM((width + SUBLANES, LANES), F32),
            pltpu.VMEM((width, 4 * LANES), BF16),
            pltpu.VMEM((width, 2 * LANES), BF16),
            pltpu.VMEM((band, band), F32),
            pltpu.VMEM((owners, 2 * own, band), F32),
            pltpu.VMEM((n, 2 * own, band), F32),
            pltpu.VMEM((tilts, owners) + message, F32),
            pltpu.VMEM((tilts, owners) + message, F32),
            pltpu.VMEM((tilts, n // 2) + message, F32),
            pltpu.VMEM(part, F32),
            pltpu.VMEM((owners,) + part, F32),
            dma((9 + planes,)),
            dma((owners,)), dma, dma, dma,
            dma((owners,)), dma((tilts,)), dma((n,)), dma((owners,)),
        ],
        compiler_params=pltpu.CompilerParams(
            collective_id=0, has_side_effects=True, vmem_limit_bytes=56 * 1024 * 1024
        ),
        name="fused",
    )(
        center, owner, shift, weight, left, share, mine,
        volume, jnp.asarray(rowt), jnp.asarray(colt),
    )


def solution(mesh):
    n = mesh.shape["slab"]

    def per_device(volume, shift, weight, left, share, center, owner, bands):
        return run(n, volume, shift, weight, left, share, center, owner, bands)

    placed = (
        P(("grp", "slab"), None, None),
        P("grp", "slab"),
        P("grp", "slab"),
        P("grp", None),
        P("grp", None),
        P("grp", None),
        P("grp"),
        P(("grp", "slab"), None, None, None),
    )
    return jax.shard_map(
        per_device,
        mesh=mesh,
        in_specs=placed,
        out_specs=(P("grp", "slab", None), P("grp")),
        check_vma=False,
    )
```

```python
import functools
import math

import jax
import jax.numpy as jnp
import numpy as np
from jax import lax
from jax.experimental import pallas as pl
from jax.experimental.pallas import tpu as pltpu
from jax.sharding import PartitionSpec as P

MESH = pl.DeviceIdType.MESH
LANES = 128
SUBLANES = 8
CHUNK = 256
OWNERS = 4
PIECES = 4
BF16 = jnp.bfloat16
F32 = jnp.float32


def phases(left, right, length):
    angle = (np.outer(left, right) % length) * (2.0 * math.pi / length)
    return np.cos(angle), np.sin(angle)


def split(values):
    high = values.astype(np.float32).astype(BF16)
    low = (values - high.astype(np.float64)).astype(np.float32).astype(BF16)
    return high, low


def halves(value):
    high = value.astype(BF16)
    return high, (value - high.astype(F32)).astype(BF16)


def row_table(length, band):
    half = band // 2
    cos, sin = phases(np.arange(half + 1), np.arange(length), length)
    last = np.zeros((SUBLANES, length))
    last[0] = sin[half]
    return np.concatenate(split(np.concatenate([cos[:half], cos[half:], sin[1:half], last])))


def col_table(length, band, owners):
    cos, sin = phases(np.arange(band), np.arange(length), length)
    own = band // owners
    rows = []
    for w in range(owners):
        rows += [cos[w * own : (w + 1) * own], sin[w * own : (w + 1) * own]]
    return np.concatenate(split(np.concatenate(rows)))


def fused_kernel(
    n, owners, center_hbm, owner_hbm, shift_hbm, weight_hbm,
    left_ref, share_ref, mine_ref, volume_ref, rowt_ref, colt_ref, out_ref,
    center_ref, owner_ref, shift_ref, weight_ref, left, share, mine, vol, rowt, colt,
    onehot, shares, rows, extra, line, summed, give, take, stack, proj,
    perm, line_keep, line_give, line_take, ref_out, ref_in, spec_out, spec_in, part_out, part_in,
    sems, ref_send, ref_recv, sib_send, sib_recv, line_send, line_recv,
    spec_send, spec_recv, part_send, part_recv,
):
    me = lax.axis_index("slab")
    core = lax.rem(me, 2)
    sibling = me + 1 - 2 * core
    chip = me // 2
    planes, height, width = volume_ref.shape
    tilts = left_ref.shape[0]
    pairs = tilts // 2
    band = mine_ref.shape[-1]
    half = band // 2
    own = band // owners
    blocks = width // LANES
    chunks = width // CHUNK
    pieces = give.shape[1]
    count = rowt_ref.shape[0] // 2
    pad = (rows.shape[1] - width) // 2
    length = width
    win_cols = out_ref.shape[-1]
    first, stride = n // owners + 1, max(2, n // (2 * owners))
    places = [first + w * stride for w in range(owners)]

    barrier = pltpu.get_barrier_semaphore()
    for k in range(1, n):
        pl.semaphore_signal(
            barrier, inc=1, device_id={"slab": lax.rem(me + k, n)}, device_id_type=MESH
        )

    def local(source, into, k):
        copy = pltpu.make_async_copy(source, into, sems.at[k])
        copy.start()
        return copy

    get_left = local(left_ref, left, 0)
    get_share = local(share_ref, share, 1)
    scalars = [
        local(shift_hbm, shift_ref, 2), local(weight_hbm, weight_ref, 3),
        local(center_hbm, center_ref, 4), local(owner_hbm, owner_ref, 5),
    ]
    get_table = local(rowt_ref, rowt, 6)
    get_mine = local(mine_ref, mine, 7)
    for z in range(planes):
        for c in range(chunks):
            part = (z, pl.ds(c * (height // chunks), height // chunks))
            local(volume_ref.at[part], vol.at[part], 9 + z)
    get_colt = local(colt_ref, colt, 8)

    def remote(source, into, send, recv, device):
        return pltpu.make_async_remote_copy(
            src_ref=source, dst_ref=into, send_sem=send, recv_sem=recv,
            device_id={"slab": device}, device_id_type=MESH,
        )

    for z in range(planes):
        rows[z, :pad, :] = jnp.zeros((pad, LANES), F32)
        rows[z, pad + width :, :] = jnp.zeros((pad, LANES), F32)
    summed[width:, :] = jnp.zeros((SUBLANES, LANES), F32)

    def row_of(ref, t, here):
        value = ref[0:1, here]
        for k in range(1, tilts):
            value = jnp.where(t == k, ref[k : k + 1, here], value)
        return value

    lane = lax.broadcasted_iota(jnp.int32, (LANES, LANES), 1)
    get_left.wait()
    get_share.wait()

    @pl.loop(0, blocks)
    def _(b):
        begin = pl.multiple_of(b * LANES, LANES)
        for i in range(pairs):
            t = 2 * i + core
            row = row_of(left, t, pl.ds(begin, LANES)).astype(F32)
            column = jnp.broadcast_to(row, (LANES, LANES)).T.astype(jnp.int32)
            for x in range(blocks):
                hit = jnp.where(column == lane + x * LANES, 1.0, 0.0)
                onehot[i, pl.ds(begin, LANES), x * LANES : (x + 1) * LANES] = hit.astype(BF16)
            row = row_of(share, t, pl.ds(begin, LANES))
            shares[i, pl.ds(begin, LANES), :] = jnp.broadcast_to(row, (LANES, LANES)).T

    get_mine.wait()
    for part in range(2):
        perm[:half, :] = mine[0, part, half:, :]
        for k in range(half):
            row = half - k if k else 0
            perm[half + k : half + k + 1, :] = mine[0, part, row : row + 1, :]
        turned = perm[...].T
        for w in range(owners):
            ref_out[w, part * own : (part + 1) * own, :] = turned[w * own : (w + 1) * own]

    def last_row(t):
        base = jnp.concatenate(
            [row_of(left, t, slice(b * LANES, (b + 1) * LANES)) for b in range(blocks)], axis=0
        )
        right = jnp.concatenate(
            [row_of(share, t, slice(b * LANES, (b + 1) * LANES)) for b in range(blocks)], axis=0
        )
        value = None
        for z in range(planes):
            weight = weight_ref[t, z]
            taps = (
                (1, right * (1.0 - weight)),
                (0, (1.0 - right) * (1.0 - weight) + right * weight),
                (-1, (1.0 - right) * weight),
            )
            for step, factor in taps:
                index = base + (step - shift_ref[t, z])
                spot = index & (LANES - 1)
                block = lax.shift_right_arithmetic(index, int(math.log2(LANES)))
                found = jnp.zeros((blocks, LANES), F32)
                for b in range(blocks):
                    source = jnp.broadcast_to(extra[z, b : b + 1, :], (blocks, LANES))
                    source = jnp.take_along_axis(source, spot, axis=1)
                    found = jnp.where(block == b, source, found)
                value = factor * found if value is None else value + factor * found
        return value

    def shifted(t, begin, size):
        total = None
        for z in range(planes):
            weight = weight_ref[t, z]
            start = pad + begin - shift_ref[t, z]
            near = rows[z, pl.ds(start, size), :]
            far = rows[z, pl.ds(start - 1, size), :]
            term = (1.0 - weight) * near + weight * far
            total = term if total is None else total + term
        return total

    def along(left_hand, right_hand):
        return lax.dot_general(
            left_hand, right_hand, (((1,), (1,)), ((), ())), preferred_element_type=F32
        )

    def to_sibling(i, k):
        return remote(
            give.at[i, k], take.at[i, k], sib_send.at[i], sib_recv.at[i, k], sibling
        )

    def to_owner(i, w):
        used = pl.ds(0, 2 * own + 1)
        t = 2 * i + core
        return remote(
            spec_out.at[i, w, used], spec_in.at[t, chip, used],
            spec_send.at[i], spec_recv.at[t], places[w],
        )

    def to_others(make):
        for w in range(owners):
            pl.when(me != places[w])(lambda: make(w).start())

    refs = pl.ds(0, 2 * own)

    def ref_to(w):
        return remote(ref_out.at[w], ref_in.at[me, refs], ref_send, ref_recv, places[w])

    span = width // pieces

    def row_chunk(z, c):
        out = jnp.dot(
            rowt[...], vol[z, :, c * CHUNK : (c + 1) * CHUNK], preferred_element_type=F32
        )
        out = out[:count] + out[count:]
        for b in range(CHUNK // LANES):
            here = slice(b * LANES, (b + 1) * LANES)
            begin = c * CHUNK + b * LANES
            rows[z, pad + begin : pad + begin + LANES, :] = out[:band, here].T
            extra[z, begin // LANES : begin // LANES + 1, :] = out[band : band + 1, here]

    def give_piece(k):
        for i in range(pairs):
            for b in range(span // LANES):
                here = slice(b * LANES, (b + 1) * LANES)
                give[i, k, here, :] = shifted(2 * i + 1 - core, k * span + b * LANES, LANES)
            to_sibling(i, k).start()

    def own_part(i):
        t = 2 * i + core
        for b in range(blocks):
            summed[b * LANES : (b + 1) * LANES, :] = shifted(t, b * LANES, LANES)

    def line_copy(i):
        return remote(line_give.at[i], line_take.at[i], line_send.at[i], line_recv.at[i], sibling)

    def last_line(i):
        line[...] = jnp.zeros(line.shape, F32)
        for k, t in enumerate((2 * i + core, 2 * i + 1 - core)):
            value = last_row(t)
            for b in range(blocks):
                line[k : k + 1, b * LANES : (b + 1) * LANES] = value[b : b + 1, :]
        value = line[...]
        high = value.astype(BF16).astype(F32)
        value = jnp.concatenate([high, value - high], axis=0).astype(BF16)
        one = along(value, colt[: 2 * band, :])
        two = along(value, colt[2 * band :, :])
        value = one[:SUBLANES] + one[SUBLANES:] + two[:SUBLANES]
        line_give[i] = jnp.zeros((SUBLANES, LANES), F32)
        for k in range(2 * band // LANES):
            here = slice(k * LANES, (k + 1) * LANES)
            line_keep[i, k : k + 1, :] = value[0:1, here]
            line_give[i, k : k + 1, :] = value[1:2, here]
        line_copy(i).start()

    def merge(i):
        def near(b):
            here = slice(b * LANES, (b + 1) * LANES)
            begin = (b * LANES) % span
            total = summed[here, :] + take[i, b * LANES // span, begin : begin + LANES, :]
            summed[here, :] = total
            high, low = halves(total)
            stack[here, 0:LANES] = high
            stack[here, LANES : 2 * LANES] = low

        def far(b):
            here = slice(b * LANES, (b + 1) * LANES)
            high, low = halves(summed[b * LANES + 1 : (b + 1) * LANES + 1, :])
            stack[here, 2 * LANES : 3 * LANES] = high
            stack[here, 3 * LANES :] = low

        each = span // LANES
        for k in range(pieces):
            to_sibling(i, k).wait_recv()
            for b in range(k * each, (k + 1) * each):
                near(b)
                if b:
                    far(b - 1)
        far(blocks - 1)

    def put_line(i):
        line_copy(i).wait_recv()
        for w in range(owners):
            begin = w * 2 * own
            offset = begin % LANES
            k = begin // LANES
            block = line_keep[i, k : k + 1, :] + line_take[i, k : k + 1, :]
            if offset:
                block = pltpu.roll(jnp.broadcast_to(block, (SUBLANES, LANES)), LANES - offset, 1)
            spec_out[i, w, 2 * own : 2 * own + 1, :] = block[0:1]

    def gather(i):
        for c in range(chunks):
            here = slice(c * CHUNK, (c + 1) * CHUNK)
            picked = jnp.dot(onehot[i, here, :], stack[...], preferred_element_type=F32)
            near = picked[:, :LANES] + picked[:, LANES : 2 * LANES]
            far = picked[:, 2 * LANES : 3 * LANES] + picked[:, 3 * LANES :]
            part = shares[i, here, :]
            high, low = halves((1.0 - part) * near + part * far)
            proj[here, :LANES] = high
            proj[here, LANES:] = low

    def columns(i):
        both = jnp.dot(colt[...], proj[...], preferred_element_type=F32)
        top = 2 * band
        value = both[:top, :LANES] + both[:top, LANES:] + both[top:, :LANES]
        for w in range(owners):
            spec_out[i, w, : 2 * own, :] = value[w * 2 * own : (w + 1) * 2 * own]

    for copy in scalars:
        copy.wait()
    get_table.wait()
    sent = 0
    for z in range(planes):
        pltpu.make_async_copy(volume_ref.at[z], vol.at[z], sems.at[9 + z]).wait()
        for c in range(chunks):
            row_chunk(z, c)
            if z == planes - 1 and c >= chunks // 2:
                if not sent:
                    pl.semaphore_wait(barrier, n - 1)
                ready = pieces if c == chunks - 1 else c * CHUNK // span
                for k in range(sent, ready):
                    give_piece(k)
                sent = ready
    to_others(ref_to)
    get_colt.wait()
    for i in range(pairs):
        last_line(i)
    for i in range(pairs):
        own_part(i)
        merge(i)
        gather(i)
        columns(i)
        put_line(i)
        to_others(functools.partial(to_owner, i))

    def wave(ints):
        angle = (ints & (length - 1)).astype(F32) * (2.0 * math.pi / length)
        return jnp.cos(angle), jnp.sin(angle)

    def thirds(value, axis, order):
        high = value.astype(BF16)
        parts = (high, (value - high.astype(F32)).astype(BF16))
        return jnp.concatenate([parts[k] for k in order], axis=axis)

    is_owner = functools.reduce(jnp.logical_or, [me == place for place in places])
    slot = (me - first) // stride

    @pl.when(is_owner)
    def _():
        spot = lax.broadcasted_iota(jnp.int32, (n, band), 1)
        freq = jnp.where(spot < half, spot, jnp.where(spot == half, -half, half - spot))
        step = lax.broadcasted_iota(jnp.int32, (n, band), 0) - n // 2
        cols = lax.broadcasted_iota(jnp.int32, (own, win_cols), 0) + slot * own
        offset = lax.broadcasted_iota(jnp.int32, (own, win_cols), 1) - win_cols // 2
        row_waves, col_waves = [], []
        for t in range(tilts):
            waves = jnp.concatenate(wave(freq * (center_ref[t, 0] + step)), axis=0)
            row_waves.append(thirds(waves, 1, (0, 0, 1)))
            cos, sin = wave(cols * (center_ref[t, 1] + offset))
            col_waves.append(thirds(jnp.concatenate([cos, -sin], axis=0), 0, (0, 1, 0)))
        spot = lax.broadcasted_iota(jnp.int32, (own, band), 1)
        lower, start, middle = spot < half, spot == 0, spot == half
        ref_in[me, refs] = ref_out[slot]
        arrived = ref_in.at[pl.ds(0, n - 1), refs]
        remote(arrived, arrived, ref_send, ref_recv, me).wait_recv()
        part_out[tilts * n :, :] = jnp.zeros((SUBLANES, win_cols), F32)

        def put_power(real, imag, row):
            power = jnp.sum(real * real + imag * imag, axis=0, keepdims=True)
            part_out[tilts * n + row : tilts * n + row + 1, :] = power

        owned = [ref_in[owner_ref[t], refs] for t in range(tilts)]
        for t in range(tilts):
            put_power(owned[t][:own], owned[t][own:], tilts + t)
        used = pl.ds(0, 2 * own + 1)
        for t in [*range(1, tilts, 2), *range(0, tilts, 2)]:
            remote_count = n // 2
            if t % 2 == 1:
                spec_in[t, chip, used] = spec_out[t // 2, slot, used]
                remote_count -= 1
            arrived = spec_in.at[t, pl.ds(0, remote_count), used]
            remote(arrived, arrived, spec_send.at[0], spec_recv.at[t], me).wait_recv()
        for t in range(tilts):
            total = spec_in[t, 0, : 2 * own]
            last = spec_in[t, 0, 2 * own : 2 * own + 1]
            for e in range(1, n // 2):
                total = total + spec_in[t, e, : 2 * own]
                last = last + spec_in[t, e, 2 * own : 2 * own + 1]
            cos, sin = total[:own], total[own:]
            last = jnp.broadcast_to(last, (SUBLANES, band)).T[:, 0:1]
            last_cos, last_sin = last[:own], last[own : 2 * own]
            cos_turn = pltpu.roll(cos, half, 1)
            sin_turn = pltpu.roll(sin, half, 1)
            spec_re = jnp.where(
                lower,
                cos - jnp.where(start, 0.0, sin_turn),
                jnp.where(middle, cos + last_sin, cos_turn + sin),
            )
            spec_im = jnp.where(
                lower,
                -(jnp.where(start, 0.0, cos_turn) + sin),
                jnp.where(middle, last_cos - sin, cos - sin_turn),
            )
            ref_re, ref_im = owned[t][:own], owned[t][own:]
            cross_re = spec_re * ref_re + spec_im * ref_im
            cross_im = spec_im * ref_re - spec_re * ref_im
            put_power(spec_re, spec_im, t)
            turned = along(
                row_waves[t],
                thirds(jnp.concatenate([cross_re, cross_im], axis=0), 1, (0, 1, 0)),
            )
            moved_re = turned[:n, :own] - turned[n:, own:]
            moved_im = turned[:n, own:] + turned[n:, :own]
            part_out[t * n : (t + 1) * n, :] = jnp.dot(
                thirds(jnp.concatenate([moved_re, moved_im], axis=1), 1, (0, 0, 1)),
                col_waves[t], preferred_element_type=F32,
            )
        for d in range(n):
            @pl.when(me != d)
            def _():
                remote(part_out, part_in.at[slot], part_send, part_recv, d).start()
        part_in[slot] = part_out[...]

    def settle(ref, send, recv, sending):
        for fewer in range(2):
            @pl.when(is_owner == (fewer == 1))
            def _():
                part = ref.at[pl.ds(0, owners - fewer)]
                copy = remote(part, part, send, recv, me)
                if sending:
                    copy.wait_send()
                else:
                    copy.wait_recv()

    settle(part_in, part_send, part_recv, False)
    total = part_in[0]
    for w in range(1, owners):
        total = total + part_in[w]
    power = jnp.sum(total[tilts * n :], axis=1, keepdims=True) / (band * band) + 1e-06
    peaks = []
    mine_row = lax.broadcasted_iota(jnp.int32, (n, win_cols), 0) == me
    for t in range(tilts):
        scale = band * jnp.sqrt(power[t : t + 1] * power[tilts + t : tilts + t + 1])
        value = total[t * n : (t + 1) * n]
        row = jnp.sum(jnp.where(mine_row, value, 0.0), axis=0, keepdims=True)
        out_ref[t] = row / scale
        peaks.append(jnp.max(jnp.max(value, axis=0, keepdims=True), axis=1, keepdims=True) / scale)
    spot = lax.broadcasted_iota(jnp.int32, (1, win_cols), 1)
    best = jnp.broadcast_to(peaks[0], (1, win_cols))
    for t in range(1, tilts):
        best = jnp.where(spot == t, peaks[t], best)
    out_ref[tilts] = best

    settle(ref_out, ref_send, ref_recv, True)
    for i in range(pairs):
        remote(give.at[i], take.at[i], sib_send.at[i], sib_recv.at[i, 0], sibling).wait_send()
        line_copy(i).wait_send()
        settle(spec_out.at[i, :, pl.ds(0, 2 * own + 1)], spec_send.at[i], spec_recv.at[0], True)

    @pl.when(is_owner)
    def _():
        every = ref_in.at[pl.ds(0, n - 1), pl.ds(0, part_out.shape[0])]
        remote(every, every, part_send, part_recv, me).wait_send()


def finish_kernel(both_ref, corr_ref, peak_ref):
    tilts = corr_ref.shape[0]
    corr_ref[...] = both_ref[:tilts]
    peak_ref[...] = both_ref[tilts, 0, :tilts]


def run(n, volume, shift, weight, left, share, center, owner, mine):
    planes, height, width = volume.shape
    tilts = left.shape[0]
    pairs = tilts // 2
    band = mine.shape[-1]
    win_cols = band
    owners = OWNERS
    rowt = row_table(height, band)
    colt = col_table(width, band, owners)
    blocks = width // LANES
    pad = width // 16 + SUBLANES
    own = band // owners
    message = (2 * own + SUBLANES, band)
    part = (tilts * n + SUBLANES, win_cols)
    smem = pl.BlockSpec(memory_space=pltpu.SMEM)
    vmem = pl.BlockSpec(memory_space=pltpu.VMEM)
    hbm = pl.BlockSpec(memory_space=pl.ANY)
    dma = pltpu.SemaphoreType.DMA
    both = pl.pallas_call(
        functools.partial(fused_kernel, n, owners),
        out_shape=pltpu.VMEM((tilts + 1, 1, win_cols), F32),
        in_specs=[hbm] * 10,
        out_specs=vmem,
        scratch_shapes=[
            pltpu.SMEM(center.shape, jnp.int32),
            pltpu.SMEM(owner.shape, jnp.int32),
            pltpu.SMEM(shift.shape, jnp.int32),
            pltpu.SMEM(weight.shape, F32),
            pltpu.VMEM(left.shape, jnp.int32),
            pltpu.VMEM(share.shape, F32),
            pltpu.VMEM(mine.shape, F32),
            pltpu.VMEM((planes, height, width), BF16),
            pltpu.VMEM(rowt.shape, BF16),
            pltpu.VMEM(colt.shape, BF16),
            pltpu.VMEM((pairs, width, width), BF16),
            pltpu.VMEM((pairs, width, LANES), F32),
            pltpu.VMEM((planes, width + 2 * pad, LANES), F32),
            pltpu.VMEM((planes, blocks, LANES), F32),
            pltpu.VMEM((SUBLANES, width), F32),
            pltpu.VMEM((width + SUBLANES, LANES), F32),
            pltpu.VMEM((pairs, PIECES, width // PIECES, LANES), F32),
            pltpu.VMEM((pairs, PIECES, width // PIECES, LANES), F32),
            pltpu.VMEM((width, 4 * LANES), BF16),
            pltpu.VMEM((width, 2 * LANES), BF16),
            pltpu.VMEM((band, band), F32),
            pltpu.VMEM((pairs, SUBLANES, LANES), F32),
            pltpu.VMEM((pairs, SUBLANES, LANES), F32),
            pltpu.VMEM((pairs, SUBLANES, LANES), F32),
            pltpu.VMEM((owners, 2 * own, band), F32),
            pltpu.VMEM((n, max(2 * own, part[0]), band), F32),
            pltpu.VMEM((pairs, owners) + message, F32),
            pltpu.VMEM((tilts, n // 2) + message, F32),
            pltpu.VMEM(part, F32),
            pltpu.VMEM((owners,) + part, F32),
            dma((9 + planes,)),
            dma, dma, dma((pairs,)), dma((pairs, PIECES)), dma((pairs,)), dma((pairs,)),
            dma((pairs,)), dma((tilts,)), dma, dma,
        ],
        compiler_params=pltpu.CompilerParams(
            collective_id=0, has_side_effects=True, vmem_limit_bytes=56 * 1024 * 1024
        ),
        name="fused",
    )(
        center, owner, shift, weight, left, share, mine,
        volume, jnp.asarray(rowt), jnp.asarray(colt),
    )
    both = pltpu.with_memory_space_constraint(both, pltpu.VMEM)
    return pl.pallas_call(
        finish_kernel,
        out_shape=(
            jax.ShapeDtypeStruct((tilts, 1, win_cols), F32),
            jax.ShapeDtypeStruct((tilts,), F32),
        ),
        in_specs=[vmem],
        out_specs=(vmem, vmem),
        name="finish",
    )(both)


def solution(mesh):
    n = mesh.shape["slab"]

    def per_device(volume, shift, weight, left, share, center, owner, bands):
        return run(n, volume, shift, weight, left, share, center, owner, bands)

    placed = (
        P(("grp", "slab"), None, None),
        P("grp", "slab"),
        P("grp", "slab"),
        P("grp", None),
        P("grp", None),
        P("grp", None),
        P("grp"),
        P(("grp", "slab"), None, None, None),
    )
    return jax.shard_map(
        per_device,
        mesh=mesh,
        in_specs=placed,
        out_specs=(P("grp", "slab", None), P("grp")),
        check_vma=False,
    )
```

```python
import functools
import math

import jax
import jax.numpy as jnp
import numpy as np
from jax import lax
from jax.experimental import pallas as pl
from jax.experimental.pallas import tpu as pltpu
from jax.sharding import PartitionSpec as P

MESH = pl.DeviceIdType.MESH
LANES = 128
SUBLANES = 8
CHUNK = 256
OWNERS = 4
PIECES = 8
HALVES = 2
BF16 = jnp.bfloat16
F32 = jnp.float32


def phases(left, right, length):
    angle = (np.outer(left, right) % length) * (2.0 * math.pi / length)
    return np.cos(angle), np.sin(angle)


def split(values):
    high = values.astype(np.float32).astype(BF16)
    low = (values - high.astype(np.float64)).astype(np.float32).astype(BF16)
    return high, low


def halves(value):
    high = value.astype(BF16)
    return high, (value - high.astype(F32)).astype(BF16)


def row_table(length, band):
    half = band // 2
    cos, sin = phases(np.arange(half + 1), np.arange(length), length)
    last = np.zeros((SUBLANES, length))
    last[0] = sin[half]
    return np.concatenate(split(np.concatenate([cos[:half], cos[half:], sin[1:half], last])))


def col_table(length, band, owners):
    cos, sin = phases(np.arange(band), np.arange(length), length)
    own = band // owners
    rows = []
    for w in range(owners):
        rows += [cos[w * own : (w + 1) * own], sin[w * own : (w + 1) * own]]
    return np.concatenate(split(np.concatenate(rows)))


def fused_kernel(
    n, owners, center_hbm, owner_hbm, shift_hbm, weight_hbm,
    left_ref, share_ref, mine_ref, volume_ref, rowt_ref, colt_ref, out_ref,
    center_ref, owner_ref, shift_ref, weight_ref, left, share, mine, vol, rowt, colt,
    onehot, shares, rows, extra, line, summed, give, take, stack, proj,
    perm, line_keep, line_give, line_take, ref_out, ref_in, spec_out, spec_in, part_out, part_in,
    sems, ref_send, ref_recv, sib_send, sib_recv, line_send, line_recv,
    spec_send, spec_recv, part_send, part_recv,
):
    me = lax.axis_index("slab")
    core = lax.rem(me, 2)
    sibling = me + 1 - 2 * core
    chip = me // 2
    planes, height, width = volume_ref.shape
    tilts = left_ref.shape[0]
    pairs = tilts // 2
    band = mine_ref.shape[-1]
    half = band // 2
    own = band // owners
    blocks = width // LANES
    chunks = width // CHUNK
    pieces = give.shape[1]
    count = rowt_ref.shape[0] // 2
    pad = (rows.shape[1] - width) // 2
    length = width
    win_cols = out_ref.shape[-1]
    first, stride = n // owners + 1, max(2, n // (2 * owners))
    places = [first + w * stride for w in range(owners)]

    is_owner = functools.reduce(jnp.logical_or, [me == place for place in places])
    beside = functools.reduce(jnp.logical_or, [sibling == place for place in places])
    barrier = pltpu.get_barrier_semaphore()

    def greet(device):
        pl.semaphore_signal(
            barrier, inc=1, device_id={"slab": device}, device_id_type=MESH
        )

    @pl.when(is_owner)
    def _():
        for k in range(1, n):
            greet(lax.rem(me + k, n))

    @pl.when(jnp.logical_not(is_owner))
    def _():
        for place in places:
            greet(place)
        pl.when(jnp.logical_not(beside))(lambda: greet(sibling))

    def wait_entry():
        others = owners + jnp.where(beside, 0, 1)
        pl.semaphore_wait(barrier, jnp.where(is_owner, n - 1, others))

    def local(source, into, k):
        copy = pltpu.make_async_copy(source, into, sems.at[k])
        copy.start()
        return copy

    def columns_of(h):
        return pl.ds(h * (width // HALVES), width // HALVES)

    get_left = local(left_ref, left, 0)
    get_share = local(share_ref, share, 1)
    scalars = [
        local(shift_hbm, shift_ref, 2), local(weight_hbm, weight_ref, 3),
        local(center_hbm, center_ref, 4), local(owner_hbm, owner_ref, 5),
    ]
    get_table = local(rowt_ref, rowt, 6)
    for h in range(HALVES):
        for z in range(planes):
            for c in range(chunks):
                part = (z, pl.ds(c * (height // chunks), height // chunks), columns_of(h))
                local(volume_ref.at[part], vol.at[part], 9 + h)
    get_mine = local(mine_ref, mine, 7)
    get_colt = local(colt_ref, colt, 8)

    def remote(source, into, send, recv, device):
        return pltpu.make_async_remote_copy(
            src_ref=source, dst_ref=into, send_sem=send, recv_sem=recv,
            device_id={"slab": device}, device_id_type=MESH,
        )

    for z in range(planes):
        rows[z, :pad, :] = jnp.zeros((pad, LANES), F32)
        rows[z, pad + width :, :] = jnp.zeros((pad, LANES), F32)
    summed[width:, :] = jnp.zeros((SUBLANES, LANES), F32)

    def row_of(ref, t, here):
        value = ref[0:1, here]
        for k in range(1, tilts):
            value = jnp.where(t == k, ref[k : k + 1, here], value)
        return value

    lane = lax.broadcasted_iota(jnp.int32, (LANES, LANES), 1)
    get_left.wait()
    get_share.wait()

    def hits(b):
        begin = pl.multiple_of(b * LANES, LANES)
        for i in range(pairs):
            t = 2 * i + core
            row = row_of(left, t, pl.ds(begin, LANES)).astype(F32)
            column = jnp.broadcast_to(row, (LANES, LANES)).T.astype(jnp.int32)
            for x in range(blocks):
                hit = jnp.where(column == lane + x * LANES, 1.0, 0.0)
                onehot[i, pl.ds(begin, LANES), x * LANES : (x + 1) * LANES] = hit.astype(BF16)
            row = row_of(share, t, pl.ds(begin, LANES))
            shares[i, pl.ds(begin, LANES), :] = jnp.broadcast_to(row, (LANES, LANES)).T

    pl.loop(0, blocks)(hits)

    def prepare_ref():
        get_mine.wait()
        for part in range(2):
            perm[:half, :] = mine[0, part, half:, :]
            for k in range(half):
                row = half - k if k else 0
                perm[half + k : half + k + 1, :] = mine[0, part, row : row + 1, :]
            turned = perm[...].T
            for w in range(owners):
                ref_out[w, part * own : (part + 1) * own, :] = turned[w * own : (w + 1) * own]

    def last_row(t):
        base = jnp.concatenate(
            [row_of(left, t, slice(b * LANES, (b + 1) * LANES)) for b in range(blocks)], axis=0
        )
        right = jnp.concatenate(
            [row_of(share, t, slice(b * LANES, (b + 1) * LANES)) for b in range(blocks)], axis=0
        )
        value = None
        for z in range(planes):
            weight = weight_ref[t, z]
            taps = (
                (1, right * (1.0 - weight)),
                (0, (1.0 - right) * (1.0 - weight) + right * weight),
                (-1, (1.0 - right) * weight),
            )
            for step, factor in taps:
                index = base + (step - shift_ref[t, z])
                spot = index & (LANES - 1)
                block = lax.shift_right_arithmetic(index, int(math.log2(LANES)))
                found = jnp.zeros((blocks, LANES), F32)
                for b in range(blocks):
                    source = jnp.broadcast_to(extra[z, b : b + 1, :], (blocks, LANES))
                    source = jnp.take_along_axis(source, spot, axis=1)
                    found = jnp.where(block == b, source, found)
                value = factor * found if value is None else value + factor * found
        return value

    def shifted(t, begin, size):
        total = None
        for z in range(planes):
            weight = weight_ref[t, z]
            start = pad + begin - shift_ref[t, z]
            near = rows[z, pl.ds(start, size), :]
            far = rows[z, pl.ds(start - 1, size), :]
            term = (1.0 - weight) * near + weight * far
            total = term if total is None else total + term
        return total

    def along(left_hand, right_hand):
        return lax.dot_general(
            left_hand, right_hand, (((1,), (1,)), ((), ())), preferred_element_type=F32
        )

    def to_sibling(i, k):
        return remote(
            give.at[i, k], take.at[i, k], sib_send.at[i], sib_recv.at[i, k], sibling
        )

    def to_owner(i, w):
        used = pl.ds(0, 2 * own + 1)
        t = 2 * i + core
        return remote(
            spec_out.at[i, w, used], spec_in.at[t, chip, used],
            spec_send.at[i], spec_recv.at[t], places[w],
        )

    def to_others(make):
        for w in range(owners):
            pl.when(me != places[w])(lambda: make(w).start())

    refs = pl.ds(0, 2 * own)

    def ref_to(w):
        return remote(ref_out.at[w], ref_in.at[me, refs], ref_send, ref_recv, places[w])

    span = width // pieces

    def row_chunk(z, c):
        out = jnp.dot(
            rowt[...], vol[z, :, c * CHUNK : (c + 1) * CHUNK], preferred_element_type=F32
        )
        out = out[:count] + out[count:]
        for b in range(CHUNK // LANES):
            here = slice(b * LANES, (b + 1) * LANES)
            begin = c * CHUNK + b * LANES
            rows[z, pad + begin : pad + begin + LANES, :] = out[:band, here].T
            extra[z, begin // LANES : begin // LANES + 1, :] = out[band : band + 1, here]

    def give_piece(k):
        for i in range(pairs):
            for b in range(span // LANES):
                here = slice(b * LANES, (b + 1) * LANES)
                give[i, k, here, :] = shifted(2 * i + 1 - core, k * span + b * LANES, LANES)
            to_sibling(i, k).start()

    def own_part(i):
        t = 2 * i + core
        for b in range(blocks):
            summed[b * LANES : (b + 1) * LANES, :] = shifted(t, b * LANES, LANES)

    def line_copy(i):
        return remote(line_give.at[i], line_take.at[i], line_send.at[i], line_recv.at[i], sibling)

    def last_line(i):
        line[...] = jnp.zeros(line.shape, F32)
        for k, t in enumerate((2 * i + core, 2 * i + 1 - core)):
            value = last_row(t)
            for b in range(blocks):
                line[k : k + 1, b * LANES : (b + 1) * LANES] = value[b : b + 1, :]
        value = line[...]
        high = value.astype(BF16).astype(F32)
        value = jnp.concatenate([high, value - high], axis=0).astype(BF16)
        one = along(value, colt[: 2 * band, :])
        two = along(value, colt[2 * band :, :])
        value = one[:SUBLANES] + one[SUBLANES:] + two[:SUBLANES]
        line_give[i] = jnp.zeros((SUBLANES, LANES), F32)
        for k in range(2 * band // LANES):
            here = slice(k * LANES, (k + 1) * LANES)
            line_keep[i, k : k + 1, :] = value[0:1, here]
            line_give[i, k : k + 1, :] = value[1:2, here]
        line_copy(i).start()

    def merge(i):
        def near(b):
            here = slice(b * LANES, (b + 1) * LANES)
            begin = (b * LANES) % span
            total = summed[here, :] + take[i, b * LANES // span, begin : begin + LANES, :]
            summed[here, :] = total
            high, low = halves(total)
            stack[here, 0:LANES] = high
            stack[here, LANES : 2 * LANES] = low

        def far(b):
            here = slice(b * LANES, (b + 1) * LANES)
            high, low = halves(summed[b * LANES + 1 : (b + 1) * LANES + 1, :])
            stack[here, 2 * LANES : 3 * LANES] = high
            stack[here, 3 * LANES :] = low

        each = span // LANES
        for k in range(pieces):
            to_sibling(i, k).wait_recv()
            for b in range(k * each, (k + 1) * each):
                near(b)
                if b:
                    far(b - 1)
        far(blocks - 1)

    def put_line(i):
        line_copy(i).wait_recv()
        for w in range(owners):
            begin = w * 2 * own
            offset = begin % LANES
            k = begin // LANES
            block = line_keep[i, k : k + 1, :] + line_take[i, k : k + 1, :]
            if offset:
                block = pltpu.roll(jnp.broadcast_to(block, (SUBLANES, LANES)), LANES - offset, 1)
            spec_out[i, w, 2 * own : 2 * own + 1, :] = block[0:1]

    def gather(i):
        for c in range(chunks):
            here = slice(c * CHUNK, (c + 1) * CHUNK)
            picked = jnp.dot(onehot[i, here, :], stack[...], preferred_element_type=F32)
            near = picked[:, :LANES] + picked[:, LANES : 2 * LANES]
            far = picked[:, 2 * LANES : 3 * LANES] + picked[:, 3 * LANES :]
            part = shares[i, here, :]
            high, low = halves((1.0 - part) * near + part * far)
            proj[here, :LANES] = high
            proj[here, LANES:] = low

    def columns(i):
        both = jnp.dot(colt[...], proj[...], preferred_element_type=F32)
        top = 2 * band
        value = both[:top, :LANES] + both[:top, LANES:] + both[top:, :LANES]
        for w in range(owners):
            spec_out[i, w, : 2 * own, :] = value[w * 2 * own : (w + 1) * 2 * own]

    get_table.wait()
    for copy in scalars:
        copy.wait()
    sent = 0
    for h in range(HALVES):
        part = (slice(None), slice(None), columns_of(h))
        pltpu.make_async_copy(volume_ref.at[part], vol.at[part], sems.at[9 + h]).wait()
        for z in range(planes):
            for c in range(chunks // HALVES):
                row_chunk(z, h * (chunks // HALVES) + c)
        if h == 0:
            wait_entry()
        known = (h + 1) * (width // HALVES)
        ready = pieces if known == width else (known - pad) // span
        for k in range(sent, ready):
            give_piece(k)
        sent = ready
    prepare_ref()
    to_others(ref_to)
    get_colt.wait()
    for i in range(pairs):
        last_line(i)
    for i in range(pairs):
        own_part(i)
        merge(i)
        gather(i)
        columns(i)
        put_line(i)
        to_others(functools.partial(to_owner, i))

    def wave(ints):
        angle = (ints & (length - 1)).astype(F32) * (2.0 * math.pi / length)
        return jnp.cos(angle), jnp.sin(angle)

    def thirds(value, axis, order):
        high = value.astype(BF16)
        parts = (high, (value - high.astype(F32)).astype(BF16))
        return jnp.concatenate([parts[k] for k in order], axis=axis)

    slot = (me - first) // stride

    @pl.when(is_owner)
    def _():
        spot = lax.broadcasted_iota(jnp.int32, (n, band), 1)
        freq = jnp.where(spot < half, spot, jnp.where(spot == half, -half, half - spot))
        step = lax.broadcasted_iota(jnp.int32, (n, band), 0) - n // 2
        cols = lax.broadcasted_iota(jnp.int32, (own, win_cols), 0) + slot * own
        offset = lax.broadcasted_iota(jnp.int32, (own, win_cols), 1) - win_cols // 2
        row_waves, col_waves = [], []
        for t in range(tilts):
            cos, sin = wave(freq * (center_ref[t, 0] + step))
            row_waves.append(thirds(jnp.concatenate([cos, -sin], axis=1), 1, (0, 0, 1)))
            cos, sin = wave(cols * (center_ref[t, 1] + offset))
            col_waves.append(halves(jnp.concatenate([cos, -sin], axis=0)))
        spot = lax.broadcasted_iota(jnp.int32, (own, band), 1)
        lower, start, middle = spot < half, spot == 0, spot == half
        ref_in[me, refs] = ref_out[slot]
        arrived = ref_in.at[pl.ds(0, n - 1), refs]
        remote(arrived, arrived, ref_send, ref_recv, me).wait_recv()
        part_out[tilts * n :, :] = jnp.zeros((SUBLANES, win_cols), F32)

        def put_power(real, imag, row):
            power = jnp.sum(real * real + imag * imag, axis=0, keepdims=True)
            part_out[tilts * n + row : tilts * n + row + 1, :] = power

        owned = [ref_in[owner_ref[t], refs] for t in range(tilts)]
        for t in range(tilts):
            put_power(owned[t][:own], owned[t][own:], tilts + t)
        used = pl.ds(0, 2 * own + 1)
        for t in [*range(1, tilts, 2), *range(0, tilts, 2)]:
            remote_count = n // 2
            if t % 2 == 1:
                spec_in[t, chip, used] = spec_out[t // 2, slot, used]
                remote_count -= 1
            arrived = spec_in.at[t, pl.ds(0, remote_count), used]
            remote(arrived, arrived, spec_send.at[0], spec_recv.at[t], me).wait_recv()
        for t in range(tilts):
            total = spec_in[t, 0, : 2 * own]
            last = spec_in[t, 0, 2 * own : 2 * own + 1]
            for e in range(1, n // 2):
                total = total + spec_in[t, e, : 2 * own]
                last = last + spec_in[t, e, 2 * own : 2 * own + 1]
            cos, sin = total[:own], total[own:]
            last = jnp.broadcast_to(last, (SUBLANES, band)).T[:, 0:1]
            last_cos, last_sin = last[:own], last[own : 2 * own]
            cos_turn = pltpu.roll(cos, half, 1)
            sin_turn = pltpu.roll(sin, half, 1)
            spec_re = jnp.where(
                lower,
                cos - jnp.where(start, 0.0, sin_turn),
                jnp.where(middle, cos + last_sin, cos_turn + sin),
            )
            spec_im = jnp.where(
                lower,
                -(jnp.where(start, 0.0, cos_turn) + sin),
                jnp.where(middle, last_cos - sin, cos - sin_turn),
            )
            ref_re, ref_im = owned[t][:own], owned[t][own:]
            cross_re = spec_re * ref_re + spec_im * ref_im
            cross_im = spec_im * ref_re - spec_re * ref_im
            put_power(spec_re, spec_im, t)
            cross = jnp.concatenate([
                jnp.concatenate([cross_re, cross_im], axis=1),
                jnp.concatenate([cross_im, -cross_re], axis=1),
            ], axis=0)
            high, low = halves(along(row_waves[t], thirds(cross, 1, (0, 1, 0))))
            near, far = col_waves[t]
            part_out[t * n : (t + 1) * n, :] = (
                jnp.dot(high, near, preferred_element_type=F32)
                + jnp.dot(high, far, preferred_element_type=F32)
                + jnp.dot(low, near, preferred_element_type=F32)
            )
        for d in range(n):
            @pl.when(me != d)
            def _():
                remote(part_out, part_in.at[slot], part_send, part_recv, d).start()
        part_in[slot] = part_out[...]

    def settle(ref, send, recv, sending):
        for fewer in range(2):
            @pl.when(is_owner == (fewer == 1))
            def _():
                part = ref.at[pl.ds(0, owners - fewer)]
                copy = remote(part, part, send, recv, me)
                if sending:
                    copy.wait_send()
                else:
                    copy.wait_recv()

    settle(part_in, part_send, part_recv, False)
    total = part_in[0]
    for w in range(1, owners):
        total = total + part_in[w]
    power = jnp.sum(total[tilts * n :], axis=1, keepdims=True) / (band * band) + 1e-06
    peaks = []
    mine_row = lax.broadcasted_iota(jnp.int32, (n, win_cols), 0) == me
    for t in range(tilts):
        scale = band * jnp.sqrt(power[t : t + 1] * power[tilts + t : tilts + t + 1])
        value = total[t * n : (t + 1) * n]
        row = jnp.sum(jnp.where(mine_row, value, 0.0), axis=0, keepdims=True)
        out_ref[t] = row / scale
        peaks.append(jnp.max(jnp.max(value, axis=0, keepdims=True), axis=1, keepdims=True) / scale)
    spot = lax.broadcasted_iota(jnp.int32, (1, win_cols), 1)
    best = jnp.broadcast_to(peaks[0], (1, win_cols))
    for t in range(1, tilts):
        best = jnp.where(spot == t, peaks[t], best)
    out_ref[tilts] = best

    settle(ref_out, ref_send, ref_recv, True)
    for i in range(pairs):
        remote(give.at[i], take.at[i], sib_send.at[i], sib_recv.at[i, 0], sibling).wait_send()
        line_copy(i).wait_send()
        settle(spec_out.at[i, :, pl.ds(0, 2 * own + 1)], spec_send.at[i], spec_recv.at[0], True)

    @pl.when(is_owner)
    def _():
        every = ref_in.at[pl.ds(0, n - 1), pl.ds(0, part_out.shape[0])]
        remote(every, every, part_send, part_recv, me).wait_send()


def finish_kernel(both_ref, corr_ref, peak_ref):
    tilts = corr_ref.shape[0]
    corr_ref[...] = both_ref[:tilts]
    peak_ref[...] = both_ref[tilts, 0, :tilts]


def run(n, volume, shift, weight, left, share, center, owner, mine):
    planes, height, width = volume.shape
    tilts = left.shape[0]
    pairs = tilts // 2
    band = mine.shape[-1]
    win_cols = band
    owners = OWNERS
    rowt = row_table(height, band)
    colt = col_table(width, band, owners)
    blocks = width // LANES
    pad = width // 16 + SUBLANES
    own = band // owners
    message = (2 * own + SUBLANES, band)
    part = (tilts * n + SUBLANES, win_cols)
    smem = pl.BlockSpec(memory_space=pltpu.SMEM)
    vmem = pl.BlockSpec(memory_space=pltpu.VMEM)
    hbm = pl.BlockSpec(memory_space=pl.ANY)
    dma = pltpu.SemaphoreType.DMA
    both = pl.pallas_call(
        functools.partial(fused_kernel, n, owners),
        out_shape=pltpu.VMEM((tilts + 1, 1, win_cols), F32),
        in_specs=[hbm] * 10,
        out_specs=vmem,
        scratch_shapes=[
            pltpu.SMEM(center.shape, jnp.int32),
            pltpu.SMEM(owner.shape, jnp.int32),
            pltpu.SMEM(shift.shape, jnp.int32),
            pltpu.SMEM(weight.shape, F32),
            pltpu.VMEM(left.shape, jnp.int32),
            pltpu.VMEM(share.shape, F32),
            pltpu.VMEM(mine.shape, F32),
            pltpu.VMEM((planes, height, width), BF16),
            pltpu.VMEM(rowt.shape, BF16),
            pltpu.VMEM(colt.shape, BF16),
            pltpu.VMEM((pairs, width, width), BF16),
            pltpu.VMEM((pairs, width, LANES), F32),
            pltpu.VMEM((planes, width + 2 * pad, LANES), F32),
            pltpu.VMEM((planes, blocks, LANES), F32),
            pltpu.VMEM((SUBLANES, width), F32),
            pltpu.VMEM((width + SUBLANES, LANES), F32),
            pltpu.VMEM((pairs, PIECES, width // PIECES, LANES), F32),
            pltpu.VMEM((pairs, PIECES, width // PIECES, LANES), F32),
            pltpu.VMEM((width, 4 * LANES), BF16),
            pltpu.VMEM((width, 2 * LANES), BF16),
            pltpu.VMEM((band, band), F32),
            pltpu.VMEM((pairs, SUBLANES, LANES), F32),
            pltpu.VMEM((pairs, SUBLANES, LANES), F32),
            pltpu.VMEM((pairs, SUBLANES, LANES), F32),
            pltpu.VMEM((owners, 2 * own, band), F32),
            pltpu.VMEM((n, max(2 * own, part[0]), band), F32),
            pltpu.VMEM((pairs, owners) + message, F32),
            pltpu.VMEM((tilts, n // 2) + message, F32),
            pltpu.VMEM(part, F32),
            pltpu.VMEM((owners,) + part, F32),
            dma((9 + HALVES,)),
            dma, dma, dma((pairs,)), dma((pairs, PIECES)), dma((pairs,)), dma((pairs,)),
            dma((pairs,)), dma((tilts,)), dma, dma,
        ],
        compiler_params=pltpu.CompilerParams(
            collective_id=0, has_side_effects=True, vmem_limit_bytes=56 * 1024 * 1024
        ),
        name="fused",
    )(
        center, owner, shift, weight, left, share, mine,
        volume, jnp.asarray(rowt), jnp.asarray(colt),
    )
    both = pltpu.with_memory_space_constraint(both, pltpu.VMEM)
    return pl.pallas_call(
        finish_kernel,
        out_shape=(
            jax.ShapeDtypeStruct((tilts, 1, win_cols), F32),
            jax.ShapeDtypeStruct((tilts,), F32),
        ),
        in_specs=[vmem],
        out_specs=(vmem, vmem),
        name="finish",
    )(both)


def solution(mesh):
    n = mesh.shape["slab"]

    def per_device(volume, shift, weight, left, share, center, owner, bands):
        return run(n, volume, shift, weight, left, share, center, owner, bands)

    placed = (
        P(("grp", "slab"), None, None),
        P("grp", "slab"),
        P("grp", "slab"),
        P("grp", None),
        P("grp", None),
        P("grp", None),
        P("grp"),
        P(("grp", "slab"), None, None, None),
    )
    return jax.shard_map(
        per_device,
        mesh=mesh,
        in_specs=placed,
        out_specs=(P("grp", "slab", None), P("grp")),
        check_vma=False,
    )
```

```python
import functools
import math

import jax
import jax.numpy as jnp
import numpy as np
from jax import lax
from jax.experimental import pallas as pl
from jax.experimental.pallas import tpu as pltpu
from jax.sharding import PartitionSpec as P

MESH = pl.DeviceIdType.MESH
LANES = 128
SUBLANES = 8
CHUNK = 256
OWNERS = 4
PIECES = 8
STOPS = (4, 8)
PARTS = (3, 4)
BF16 = jnp.bfloat16
F32 = jnp.float32


def phases(left, right, length):
    angle = (np.outer(left, right) % length) * (2.0 * math.pi / length)
    return np.cos(angle), np.sin(angle)


def split(values):
    high = values.astype(np.float32).astype(BF16)
    low = (values - high.astype(np.float64)).astype(np.float32).astype(BF16)
    return high, low


def halves(value):
    high = value.astype(BF16)
    return high, (value - high.astype(F32)).astype(BF16)


def row_table(length, band):
    half = band // 2
    cos, sin = phases(np.arange(half + 1), np.arange(length), length)
    last = np.zeros((SUBLANES, length))
    last[0] = sin[half]
    return np.concatenate(split(np.concatenate([cos[:half], cos[half:], sin[1:half], last])))


def col_table(length, band, owners):
    cos, sin = phases(np.arange(band), np.arange(length), length)
    own = band // owners
    rows = []
    for w in range(owners):
        rows += [cos[w * own : (w + 1) * own], sin[w * own : (w + 1) * own]]
    return np.concatenate(split(np.concatenate(rows)))


def fused_kernel(
    n, owners, center_hbm, owner_hbm, shift_hbm, weight_hbm,
    left_ref, share_ref, mine_ref, volume_ref, rowt_ref, colt_ref, out_ref,
    center_ref, owner_ref, shift_ref, weight_ref, left, share, mine, vol, rowt, colt,
    onehot, shares, rows, extra, line, summed, sofar, give, take, stack, proj,
    perm, line_keep, line_give, line_take, ref_out, ref_in, spec_out, spec_in, part_out, part_in,
    sems, ref_send, ref_recv, sib_send, sib_recv, line_send, line_recv,
    spec_send, spec_recv, part_send, part_recv,
):
    me = lax.axis_index("slab")
    core = lax.rem(me, 2)
    sibling = me + 1 - 2 * core
    chip = me // 2
    planes, height, width = volume_ref.shape
    tilts = left_ref.shape[0]
    pairs = tilts // 2
    band = mine_ref.shape[-1]
    half = band // 2
    own = band // owners
    blocks = width // LANES
    chunks = width // CHUNK
    pieces = give.shape[1]
    count = rowt_ref.shape[0] // 2
    pad = (rows.shape[1] - width) // 2
    length = width
    win_cols = out_ref.shape[-1]
    first, stride = n // owners + 1, max(2, n // (2 * owners))
    places = [first + w * stride for w in range(owners)]

    is_owner = functools.reduce(jnp.logical_or, [me == place for place in places])
    beside = functools.reduce(jnp.logical_or, [sibling == place for place in places])
    barrier = pltpu.get_barrier_semaphore()

    def greet(device):
        pl.semaphore_signal(
            barrier, inc=1, device_id={"slab": device}, device_id_type=MESH
        )

    def wait_entry():
        others = owners + jnp.where(beside, 0, 1)
        pl.semaphore_wait(barrier, jnp.where(is_owner, n - 1, others))

    def local(source, into, k):
        copy = pltpu.make_async_copy(source, into, sems.at[k])
        copy.start()
        return copy

    ends = [chunks * part // 4 for part in PARTS]
    begins = [0] + ends[:-1]

    def columns_of(h):
        return pl.ds(begins[h] * CHUNK, (ends[h] - begins[h]) * CHUNK)

    get_left = local(left_ref, left, 0)
    get_share = local(share_ref, share, 1)
    get_table = local(rowt_ref, rowt, 6)
    for h in range(len(PARTS)):
        for z in range(planes):
            for c in range(chunks):
                part = (z, pl.ds(c * (height // chunks), height // chunks), columns_of(h))
                local(volume_ref.at[part], vol.at[part], 9 + h)
    scalars = [
        local(shift_hbm, shift_ref, 2), local(weight_hbm, weight_ref, 3),
        local(center_hbm, center_ref, 4), local(owner_hbm, owner_ref, 5),
    ]
    get_mine = local(mine_ref, mine, 7)
    get_colt = local(colt_ref, colt, 8)

    @pl.when(is_owner)
    def _():
        for k in range(1, n):
            greet(lax.rem(me + k, n))

    @pl.when(jnp.logical_not(is_owner))
    def _():
        for place in places:
            greet(place)
        pl.when(jnp.logical_not(beside))(lambda: greet(sibling))

    def remote(source, into, send, recv, device):
        return pltpu.make_async_remote_copy(
            src_ref=source, dst_ref=into, send_sem=send, recv_sem=recv,
            device_id={"slab": device}, device_id_type=MESH,
        )

    for z in range(planes):
        rows[z, :pad, :] = jnp.zeros((pad, LANES), F32)
        rows[z, pad + width :, :] = jnp.zeros((pad, LANES), F32)
    summed[width:, :] = jnp.zeros((SUBLANES, LANES), F32)

    def row_of(ref, t, here):
        value = ref[0:1, here]
        for k in range(1, tilts):
            value = jnp.where(t == k, ref[k : k + 1, here], value)
        return value

    lane = lax.broadcasted_iota(jnp.int32, (LANES, LANES), 1)
    get_left.wait()
    get_share.wait()

    def hits(b):
        begin = pl.multiple_of(b * LANES, LANES)
        for i in range(pairs):
            t = 2 * i + core
            row = row_of(left, t, pl.ds(begin, LANES)).astype(F32)
            column = jnp.broadcast_to(row, (LANES, LANES)).T.astype(jnp.int32)
            for x in range(blocks):
                hit = jnp.where(column == lane + x * LANES, 1.0, 0.0)
                onehot[i, pl.ds(begin, LANES), x * LANES : (x + 1) * LANES] = hit.astype(BF16)
            row = row_of(share, t, pl.ds(begin, LANES))
            shares[i, pl.ds(begin, LANES), :] = jnp.broadcast_to(row, (LANES, LANES)).T

    pl.loop(0, blocks)(hits)

    def prepare_ref():
        get_mine.wait()
        for part in range(2):
            perm[:half, :] = mine[0, part, half:, :]
            for k in range(half):
                row = half - k if k else 0
                perm[half + k : half + k + 1, :] = mine[0, part, row : row + 1, :]
            turned = perm[...].T
            for w in range(owners):
                ref_out[w, part * own : (part + 1) * own, :] = turned[w * own : (w + 1) * own]

    def last_row(t):
        base = jnp.concatenate(
            [row_of(left, t, slice(b * LANES, (b + 1) * LANES)) for b in range(blocks)], axis=0
        )
        right = jnp.concatenate(
            [row_of(share, t, slice(b * LANES, (b + 1) * LANES)) for b in range(blocks)], axis=0
        )
        value = None
        for z in range(planes):
            weight = weight_ref[t, z]
            taps = (
                (1, right * (1.0 - weight)),
                (0, (1.0 - right) * (1.0 - weight) + right * weight),
                (-1, (1.0 - right) * weight),
            )
            for step, factor in taps:
                index = base + (step - shift_ref[t, z])
                spot = index & (LANES - 1)
                block = lax.shift_right_arithmetic(index, int(math.log2(LANES)))
                found = jnp.zeros((blocks, LANES), F32)
                for b in range(blocks):
                    source = jnp.broadcast_to(extra[z, b : b + 1, :], (blocks, LANES))
                    source = jnp.take_along_axis(source, spot, axis=1)
                    found = jnp.where(block == b, source, found)
                value = factor * found if value is None else value + factor * found
        return value

    def shifted(t, begin, size):
        total = None
        for z in range(planes):
            weight = weight_ref[t, z]
            start = pad + begin - shift_ref[t, z]
            near = rows[z, pl.ds(start, size), :]
            far = rows[z, pl.ds(start - 1, size), :]
            term = (1.0 - weight) * near + weight * far
            total = term if total is None else total + term
        return total

    def along(left_hand, right_hand):
        return lax.dot_general(
            left_hand, right_hand, (((1,), (1,)), ((), ())), preferred_element_type=F32
        )

    def to_sibling(i, k):
        return remote(
            give.at[i, k], take.at[i, k], sib_send.at[i], sib_recv.at[i, k], sibling
        )

    def to_owner(i, w):
        used = pl.ds(0, 2 * own + 1)
        t = 2 * i + core
        return remote(
            spec_out.at[i, w, used], spec_in.at[t, chip, used],
            spec_send.at[i], spec_recv.at[t], places[w],
        )

    def to_others(make):
        for w in reversed(range(owners)):
            pl.when(me != places[w])(lambda: make(w).start())

    refs = pl.ds(0, 2 * own)

    def ref_to(w):
        return remote(ref_out.at[w], ref_in.at[me, refs], ref_send, ref_recv, places[w])

    span = width // pieces

    def row_chunk(z, c):
        out = jnp.dot(
            rowt[...], vol[z, :, c * CHUNK : (c + 1) * CHUNK], preferred_element_type=F32
        )
        out = out[:count] + out[count:]
        for b in range(CHUNK // LANES):
            here = slice(b * LANES, (b + 1) * LANES)
            begin = c * CHUNK + b * LANES
            rows[z, pad + begin : pad + begin + LANES, :] = out[:band, here].T
            extra[z, begin // LANES : begin // LANES + 1, :] = out[band : band + 1, here]

    def give_piece(k):
        for i in range(pairs):
            for b in range(span // LANES):
                here = slice(b * LANES, (b + 1) * LANES)
                give[i, k, here, :] = shifted(2 * i + 1 - core, k * span + b * LANES, LANES)
            to_sibling(i, k).start()

    def own_part(i):
        t = 2 * i + core
        for b in range(blocks):
            summed[b * LANES : (b + 1) * LANES, :] = shifted(t, b * LANES, LANES)

    def line_copy(i):
        return remote(line_give.at[i], line_take.at[i], line_send.at[i], line_recv.at[i], sibling)

    def last_line(i):
        line[...] = jnp.zeros(line.shape, F32)
        for k, t in enumerate((2 * i + core, 2 * i + 1 - core)):
            value = last_row(t)
            for b in range(blocks):
                line[k : k + 1, b * LANES : (b + 1) * LANES] = value[b : b + 1, :]
        value = line[...]
        high = value.astype(BF16).astype(F32)
        value = jnp.concatenate([high, value - high], axis=0).astype(BF16)
        one = along(value, colt[: 2 * band, :])
        two = along(value, colt[2 * band :, :])
        value = one[:SUBLANES] + one[SUBLANES:] + two[:SUBLANES]
        line_give[i] = jnp.zeros((SUBLANES, LANES), F32)
        for k in range(2 * band // LANES):
            here = slice(k * LANES, (k + 1) * LANES)
            line_keep[i, k : k + 1, :] = value[0:1, here]
            line_give[i, k : k + 1, :] = value[1:2, here]
        line_copy(i).start()

    each = span // LANES

    def near(i, b):
        here = slice(b * LANES, (b + 1) * LANES)
        if b % each == 0:
            to_sibling(i, b // each).wait_recv()
        begin = (b % each) * LANES
        total = summed[here, :] + take[i, b // each, begin : begin + LANES, :]
        summed[here, :] = total
        high, low = halves(total)
        stack[here, 0:LANES] = high
        stack[here, LANES : 2 * LANES] = low

    def far(b):
        here = slice(b * LANES, (b + 1) * LANES)
        high, low = halves(summed[b * LANES + 1 : (b + 1) * LANES + 1, :])
        stack[here, 2 * LANES : 3 * LANES] = high
        stack[here, 3 * LANES :] = low

    def merge(i, begin, end):
        for b in range(begin + (1 if begin else 0), min(end + 1, blocks)):
            near(i, b)
            if b > begin:
                far(b - 1)
        if end == blocks:
            far(blocks - 1)

    def put_line(i):
        line_copy(i).wait_recv()
        for w in range(owners):
            begin = w * 2 * own
            offset = begin % LANES
            k = begin // LANES
            block = line_keep[i, k : k + 1, :] + line_take[i, k : k + 1, :]
            if offset:
                block = pltpu.roll(jnp.broadcast_to(block, (SUBLANES, LANES)), LANES - offset, 1)
            spec_out[i, w, 2 * own : 2 * own + 1, :] = block[0:1]

    def gather(i, begin, end):
        deep = slice(begin * LANES, end * LANES)
        for c in range(chunks):
            here = slice(c * CHUNK, (c + 1) * CHUNK)
            picked = jnp.dot(onehot[i, here, deep], stack[deep, :], preferred_element_type=F32)
            near = picked[:, :LANES] + picked[:, LANES : 2 * LANES]
            far = picked[:, 2 * LANES : 3 * LANES] + picked[:, 3 * LANES :]
            part = shares[i, here, :]
            value = (1.0 - part) * near + part * far
            if begin:
                value = value + sofar[here, :]
            if end < blocks:
                sofar[here, :] = value
            else:
                high, low = halves(value)
                proj[here, :LANES] = high
                proj[here, LANES:] = low

    def columns(i):
        both = jnp.dot(colt[...], proj[...], preferred_element_type=F32)
        top = 2 * band
        value = both[:top, :LANES] + both[:top, LANES:] + both[top:, :LANES]
        for w in range(owners):
            spec_out[i, w, : 2 * own, :] = value[w * 2 * own : (w + 1) * 2 * own]

    get_table.wait()
    for copy in scalars:
        copy.wait()
    sent = 0
    for h in range(len(PARTS)):
        part = (slice(None), slice(None), columns_of(h))
        pltpu.make_async_copy(volume_ref.at[part], vol.at[part], sems.at[9 + h]).wait()
        for z in range(planes):
            for c in range(begins[h], ends[h]):
                row_chunk(z, c)
        if h == 0:
            wait_entry()
        known = ends[h] * CHUNK
        ready = pieces if known == width else (known - pad) // span
        for k in range(sent, ready):
            give_piece(k)
        sent = ready
    prepare_ref()
    to_others(ref_to)
    get_colt.wait()
    for i in range(pairs):
        last_line(i)
    for i in range(pairs):
        own_part(i)
        stops = [blocks * stop // 8 for stop in STOPS]
        for begin, end in zip([0] + stops[:-1], stops):
            merge(i, begin, end)
            gather(i, begin, end)
        columns(i)
        put_line(i)
        to_others(functools.partial(to_owner, i))

    def wave(ints):
        angle = (ints & (length - 1)).astype(F32) * (2.0 * math.pi / length)
        return jnp.cos(angle), jnp.sin(angle)

    def thirds(value, axis, order):
        high = value.astype(BF16)
        parts = (high, (value - high.astype(F32)).astype(BF16))
        return jnp.concatenate([parts[k] for k in order], axis=axis)

    slot = (me - first) // stride

    @pl.when(is_owner)
    def _():
        spot = lax.broadcasted_iota(jnp.int32, (n, band), 1)
        freq = jnp.where(spot < half, spot, jnp.where(spot == half, -half, half - spot))
        step = lax.broadcasted_iota(jnp.int32, (n, band), 0) - n // 2
        cols = lax.broadcasted_iota(jnp.int32, (own, win_cols), 0) + slot * own
        offset = lax.broadcasted_iota(jnp.int32, (own, win_cols), 1) - win_cols // 2
        row_waves, col_waves = [], []
        for t in range(tilts):
            cos, sin = wave(freq * (center_ref[t, 0] + step))
            row_waves.append(thirds(jnp.concatenate([cos, -sin], axis=1), 1, (0, 0, 1)))
            cos, sin = wave(cols * (center_ref[t, 1] + offset))
            col_waves.append(halves(jnp.concatenate([cos, -sin], axis=0)))
        spot = lax.broadcasted_iota(jnp.int32, (own, band), 1)
        lower, start, middle = spot < half, spot == 0, spot == half
        ref_in[me, refs] = ref_out[slot]
        arrived = ref_in.at[pl.ds(0, n - 1), refs]
        remote(arrived, arrived, ref_send, ref_recv, me).wait_recv()
        part_out[tilts * n :, :] = jnp.zeros((SUBLANES, win_cols), F32)

        def put_power(real, imag, row):
            power = jnp.sum(real * real + imag * imag, axis=0, keepdims=True)
            part_out[tilts * n + row : tilts * n + row + 1, :] = power

        owned = [ref_in[owner_ref[t], refs] for t in range(tilts)]
        for t in range(tilts):
            put_power(owned[t][:own], owned[t][own:], tilts + t)
        used = pl.ds(0, 2 * own + 1)
        for t in [*range(1, tilts, 2), *range(0, tilts, 2)]:
            remote_count = n // 2
            if t % 2 == 1:
                spec_in[t, chip, used] = spec_out[t // 2, slot, used]
                remote_count -= 1
            arrived = spec_in.at[t, pl.ds(0, remote_count), used]
            remote(arrived, arrived, spec_send.at[0], spec_recv.at[t], me).wait_recv()
            total = spec_in[t, 0, : 2 * own]
            last = spec_in[t, 0, 2 * own : 2 * own + 1]
            for e in range(1, n // 2):
                total = total + spec_in[t, e, : 2 * own]
                last = last + spec_in[t, e, 2 * own : 2 * own + 1]
            cos, sin = total[:own], total[own:]
            last = jnp.broadcast_to(last, (SUBLANES, band)).T[:, 0:1]
            last_cos, last_sin = last[:own], last[own : 2 * own]
            cos_turn = pltpu.roll(cos, half, 1)
            sin_turn = pltpu.roll(sin, half, 1)
            spec_re = jnp.where(
                lower,
                cos - jnp.where(start, 0.0, sin_turn),
                jnp.where(middle, cos + last_sin, cos_turn + sin),
            )
            spec_im = jnp.where(
                lower,
                -(jnp.where(start, 0.0, cos_turn) + sin),
                jnp.where(middle, last_cos - sin, cos - sin_turn),
            )
            ref_re, ref_im = owned[t][:own], owned[t][own:]
            cross_re = spec_re * ref_re + spec_im * ref_im
            cross_im = spec_im * ref_re - spec_re * ref_im
            put_power(spec_re, spec_im, t)
            cross = jnp.concatenate([
                jnp.concatenate([cross_re, cross_im], axis=1),
                jnp.concatenate([cross_im, -cross_re], axis=1),
            ], axis=0)
            high, low = halves(along(row_waves[t], thirds(cross, 1, (0, 1, 0))))
            near, far = col_waves[t]
            part_out[t * n : (t + 1) * n, :] = (
                jnp.dot(high, near, preferred_element_type=F32)
                + jnp.dot(high, far, preferred_element_type=F32)
                + jnp.dot(low, near, preferred_element_type=F32)
            )
        for d in range(n):
            @pl.when(me != d)
            def _():
                remote(part_out, part_in.at[slot], part_send, part_recv, d).start()
        part_in[slot] = part_out[...]

    def settle(ref, send, recv, sending):
        for fewer in range(2):
            @pl.when(is_owner == (fewer == 1))
            def _():
                part = ref.at[pl.ds(0, owners - fewer)]
                copy = remote(part, part, send, recv, me)
                if sending:
                    copy.wait_send()
                else:
                    copy.wait_recv()

    settle(part_in, part_send, part_recv, False)
    total = part_in[0]
    for w in range(1, owners):
        total = total + part_in[w]
    power = jnp.sum(total[tilts * n :], axis=1, keepdims=True) / (band * band) + 1e-06
    peaks = []
    mine_row = lax.broadcasted_iota(jnp.int32, (n, win_cols), 0) == me
    for t in range(tilts):
        scale = band * jnp.sqrt(power[t : t + 1] * power[tilts + t : tilts + t + 1])
        value = total[t * n : (t + 1) * n]
        row = jnp.sum(jnp.where(mine_row, value, 0.0), axis=0, keepdims=True)
        out_ref[t] = row / scale
        peaks.append(jnp.max(jnp.max(value, axis=0, keepdims=True), axis=1, keepdims=True) / scale)
    spot = lax.broadcasted_iota(jnp.int32, (1, win_cols), 1)
    best = jnp.broadcast_to(peaks[0], (1, win_cols))
    for t in range(1, tilts):
        best = jnp.where(spot == t, peaks[t], best)
    out_ref[tilts] = best

    settle(ref_out, ref_send, ref_recv, True)
    for i in range(pairs):
        remote(give.at[i], take.at[i], sib_send.at[i], sib_recv.at[i, 0], sibling).wait_send()
        line_copy(i).wait_send()
        settle(spec_out.at[i, :, pl.ds(0, 2 * own + 1)], spec_send.at[i], spec_recv.at[0], True)

    @pl.when(is_owner)
    def _():
        every = ref_in.at[pl.ds(0, n - 1), pl.ds(0, part_out.shape[0])]
        remote(every, every, part_send, part_recv, me).wait_send()


def finish_kernel(both_ref, corr_ref, peak_ref):
    tilts = corr_ref.shape[0]
    corr_ref[...] = both_ref[:tilts]
    peak_ref[...] = both_ref[tilts, 0, :tilts]


def run(n, volume, shift, weight, left, share, center, owner, mine):
    planes, height, width = volume.shape
    tilts = left.shape[0]
    pairs = tilts // 2
    band = mine.shape[-1]
    win_cols = band
    owners = OWNERS
    rowt = row_table(height, band)
    colt = col_table(width, band, owners)
    blocks = width // LANES
    pad = width // 16 + SUBLANES
    own = band // owners
    message = (2 * own + SUBLANES, band)
    part = (tilts * n + SUBLANES, win_cols)
    smem = pl.BlockSpec(memory_space=pltpu.SMEM)
    vmem = pl.BlockSpec(memory_space=pltpu.VMEM)
    hbm = pl.BlockSpec(memory_space=pl.ANY)
    dma = pltpu.SemaphoreType.DMA
    both = pl.pallas_call(
        functools.partial(fused_kernel, n, owners),
        out_shape=pltpu.VMEM((tilts + 1, 1, win_cols), F32),
        in_specs=[hbm] * 10,
        out_specs=vmem,
        scratch_shapes=[
            pltpu.SMEM(center.shape, jnp.int32),
            pltpu.SMEM(owner.shape, jnp.int32),
            pltpu.SMEM(shift.shape, jnp.int32),
            pltpu.SMEM(weight.shape, F32),
            pltpu.VMEM(left.shape, jnp.int32),
            pltpu.VMEM(share.shape, F32),
            pltpu.VMEM(mine.shape, F32),
            pltpu.VMEM((planes, height, width), BF16),
            pltpu.VMEM(rowt.shape, BF16),
            pltpu.VMEM(colt.shape, BF16),
            pltpu.VMEM((pairs, width, width), BF16),
            pltpu.VMEM((pairs, width, LANES), F32),
            pltpu.VMEM((planes, width + 2 * pad, LANES), F32),
            pltpu.VMEM((planes, blocks, LANES), F32),
            pltpu.VMEM((SUBLANES, width), F32),
            pltpu.VMEM((width + SUBLANES, LANES), F32),
            pltpu.VMEM((width, LANES), F32),
            pltpu.VMEM((pairs, PIECES, width // PIECES, LANES), F32),
            pltpu.VMEM((pairs, PIECES, width // PIECES, LANES), F32),
            pltpu.VMEM((width, 4 * LANES), BF16),
            pltpu.VMEM((width, 2 * LANES), BF16),
            pltpu.VMEM((band, band), F32),
            pltpu.VMEM((pairs, SUBLANES, LANES), F32),
            pltpu.VMEM((pairs, SUBLANES, LANES), F32),
            pltpu.VMEM((pairs, SUBLANES, LANES), F32),
            pltpu.VMEM((owners, 2 * own, band), F32),
            pltpu.VMEM((n, max(2 * own, part[0]), band), F32),
            pltpu.VMEM((pairs, owners) + message, F32),
            pltpu.VMEM((tilts, n // 2) + message, F32),
            pltpu.VMEM(part, F32),
            pltpu.VMEM((owners,) + part, F32),
            dma((9 + len(PARTS),)),
            dma, dma, dma((pairs,)), dma((pairs, PIECES)), dma((pairs,)), dma((pairs,)),
            dma((pairs,)), dma((tilts,)), dma, dma,
        ],
        compiler_params=pltpu.CompilerParams(
            collective_id=0, has_side_effects=True, vmem_limit_bytes=56 * 1024 * 1024
        ),
        name="fused",
    )(
        center, owner, shift, weight, left, share, mine,
        volume, jnp.asarray(rowt), jnp.asarray(colt),
    )
    both = pltpu.with_memory_space_constraint(both, pltpu.VMEM)
    return pl.pallas_call(
        finish_kernel,
        out_shape=(
            jax.ShapeDtypeStruct((tilts, 1, win_cols), F32),
            jax.ShapeDtypeStruct((tilts,), F32),
        ),
        in_specs=[vmem],
        out_specs=(vmem, vmem),
        name="finish",
    )(both)


def solution(mesh):
    n = mesh.shape["slab"]

    def per_device(volume, shift, weight, left, share, center, owner, bands):
        return run(n, volume, shift, weight, left, share, center, owner, bands)

    placed = (
        P(("grp", "slab"), None, None),
        P("grp", "slab"),
        P("grp", "slab"),
        P("grp", None),
        P("grp", None),
        P("grp", None),
        P("grp"),
        P(("grp", "slab"), None, None, None),
    )
    return jax.shard_map(
        per_device,
        mesh=mesh,
        in_specs=placed,
        out_specs=(P("grp", "slab", None), P("grp")),
        check_vma=False,
    )
```

```python
import functools
import math

import jax
import jax.numpy as jnp
import numpy as np
from jax import lax
from jax.experimental import pallas as pl
from jax.experimental.pallas import tpu as pltpu
from jax.sharding import PartitionSpec as P

MESH = pl.DeviceIdType.MESH
LANES = 128
SUBLANES = 8
CHUNK = 256
OWNERS = 4
PIECES = 8
STOPS = (4, 8)
PARTS = (3, 4)
BF16 = jnp.bfloat16
F32 = jnp.float32


def phases(left, right, length):
    angle = (np.outer(left, right) % length) * (2.0 * math.pi / length)
    return np.cos(angle), np.sin(angle)


def split(values):
    high = values.astype(np.float32).astype(BF16)
    low = (values - high.astype(np.float64)).astype(np.float32).astype(BF16)
    return high, low


def halves(value):
    high = value.astype(BF16)
    return high, (value - high.astype(F32)).astype(BF16)


def row_table(length, band):
    half = band // 2
    cos, sin = phases(np.arange(half + 1), np.arange(length), length)
    last = np.zeros((SUBLANES, length))
    last[0] = sin[half]
    return np.concatenate(split(np.concatenate([cos[:half], cos[half:], sin[1:half], last])))


def col_table(length, band, owners):
    cos, sin = phases(np.arange(band), np.arange(length), length)
    own = band // owners
    rows = []
    for w in range(owners):
        rows += [cos[w * own : (w + 1) * own], sin[w * own : (w + 1) * own]]
    return np.concatenate(split(np.concatenate(rows)))


def fused_kernel(
    n, owners, center_hbm, owner_hbm, shift_hbm, weight_hbm,
    left_ref, share_ref, mine_ref, volume_ref, rowt_ref, colt_ref, out_ref,
    center_ref, owner_ref, shift_ref, weight_ref, left, share, mine, vol, rowt, colt,
    onehot, shares, rows, extra, line, summed, sofar, give, take, stack, proj,
    perm, line_keep, line_give, line_take, ref_out, ref_in, spec_out, spec_in, part_out, part_in,
    sems, ref_send, ref_recv, sib_send, sib_recv, line_send, line_recv,
    spec_send, spec_recv, part_send, part_recv,
):
    me = lax.axis_index("slab")
    core = lax.rem(me, 2)
    sibling = me + 1 - 2 * core
    chip = me // 2
    planes, height, width = volume_ref.shape
    tilts = left_ref.shape[0]
    pairs = tilts // 2
    band = mine_ref.shape[-1]
    half = band // 2
    own = band // owners
    blocks = width // LANES
    chunks = width // CHUNK
    pieces = give.shape[1]
    count = rowt_ref.shape[0] // 2
    pad = (rows.shape[1] - width) // 2
    length = width
    win_cols = out_ref.shape[-1]
    first, stride = n // owners + 1, max(2, n // (2 * owners))
    places = [first + w * stride for w in range(owners)]

    is_owner = functools.reduce(jnp.logical_or, [me == place for place in places])
    beside = functools.reduce(jnp.logical_or, [sibling == place for place in places])
    barrier = pltpu.get_barrier_semaphore()

    def greet(device):
        pl.semaphore_signal(
            barrier, inc=1, device_id={"slab": device}, device_id_type=MESH
        )

    def wait_entry():
        others = owners + jnp.where(beside, 0, 1)
        pl.semaphore_wait(barrier, jnp.where(is_owner, n - 1, others))

    def local(source, into, k):
        copy = pltpu.make_async_copy(source, into, sems.at[k])
        copy.start()
        return copy

    ends = [chunks * part // 4 for part in PARTS]
    begins = [0] + ends[:-1]

    def columns_of(h):
        return pl.ds(begins[h] * CHUNK, (ends[h] - begins[h]) * CHUNK)

    get_left = local(left_ref, left, 0)
    get_share = local(share_ref, share, 1)
    get_table = local(rowt_ref, rowt, 6)
    for h in range(len(PARTS)):
        for z in range(planes):
            for c in range(2):
                part = (z, pl.ds(c * (height // 2), height // 2), columns_of(h))
                local(volume_ref.at[part], vol.at[part], 9 + h)
    scalars = [
        local(shift_hbm, shift_ref, 2), local(weight_hbm, weight_ref, 3),
        local(center_hbm, center_ref, 4), local(owner_hbm, owner_ref, 5),
    ]
    get_mine = local(mine_ref, mine, 7)
    get_colt = local(colt_ref, colt, 8)

    @pl.when(is_owner)
    def _():
        for k in range(1, n):
            greet(lax.rem(me + k, n))

    @pl.when(jnp.logical_not(is_owner))
    def _():
        for place in places:
            greet(place)
        pl.when(jnp.logical_not(beside))(lambda: greet(sibling))

    def remote(source, into, send, recv, device):
        return pltpu.make_async_remote_copy(
            src_ref=source, dst_ref=into, send_sem=send, recv_sem=recv,
            device_id={"slab": device}, device_id_type=MESH,
        )

    for z in range(planes):
        rows[z, :pad, :] = jnp.zeros((pad, LANES), F32)
        rows[z, pad + width :, :] = jnp.zeros((pad, LANES), F32)
    summed[width:, :] = jnp.zeros((SUBLANES, LANES), F32)

    def row_of(ref, t, here):
        value = ref[0:1, here]
        for k in range(1, tilts):
            value = jnp.where(t == k, ref[k : k + 1, here], value)
        return value

    lane = lax.broadcasted_iota(jnp.int32, (LANES, LANES), 1)
    get_left.wait()
    get_share.wait()

    def hits(b):
        begin = pl.multiple_of(b * LANES, LANES)
        for i in range(pairs):
            t = 2 * i + core
            row = row_of(left, t, pl.ds(begin, LANES)).astype(F32)
            column = jnp.broadcast_to(row, (LANES, LANES)).T.astype(jnp.int32)
            for x in range(blocks):
                hit = jnp.where(column == lane + x * LANES, 1.0, 0.0)
                onehot[i, pl.ds(begin, LANES), x * LANES : (x + 1) * LANES] = hit.astype(BF16)
            row = row_of(share, t, pl.ds(begin, LANES))
            shares[i, pl.ds(begin, LANES), :] = jnp.broadcast_to(row, (LANES, LANES)).T

    pl.loop(0, blocks)(hits)

    def prepare_ref():
        get_mine.wait()
        for part in range(2):
            perm[:half, :] = mine[0, part, half:, :]
            for k in range(half):
                row = half - k if k else 0
                perm[half + k : half + k + 1, :] = mine[0, part, row : row + 1, :]
            turned = perm[...].T
            for w in range(owners):
                ref_out[w, part * own : (part + 1) * own, :] = turned[w * own : (w + 1) * own]

    def last_row(t):
        base = jnp.concatenate(
            [row_of(left, t, slice(b * LANES, (b + 1) * LANES)) for b in range(blocks)], axis=0
        )
        right = jnp.concatenate(
            [row_of(share, t, slice(b * LANES, (b + 1) * LANES)) for b in range(blocks)], axis=0
        )
        value = None
        for z in range(planes):
            weight = weight_ref[t, z]
            taps = (
                (1, right * (1.0 - weight)),
                (0, (1.0 - right) * (1.0 - weight) + right * weight),
                (-1, (1.0 - right) * weight),
            )
            for step, factor in taps:
                index = base + (step - shift_ref[t, z])
                spot = index & (LANES - 1)
                block = lax.shift_right_arithmetic(index, int(math.log2(LANES)))
                found = jnp.zeros((blocks, LANES), F32)
                for b in range(blocks):
                    source = jnp.broadcast_to(extra[z, b : b + 1, :], (blocks, LANES))
                    source = jnp.take_along_axis(source, spot, axis=1)
                    found = jnp.where(block == b, source, found)
                value = factor * found if value is None else value + factor * found
        return value

    def shifted(t, begin, size):
        total = None
        for z in range(planes):
            weight = weight_ref[t, z]
            start = pad + begin - shift_ref[t, z]
            near = rows[z, pl.ds(start, size), :]
            far = rows[z, pl.ds(start - 1, size), :]
            term = (1.0 - weight) * near + weight * far
            total = term if total is None else total + term
        return total

    def along(left_hand, right_hand):
        return lax.dot_general(
            left_hand, right_hand, (((1,), (1,)), ((), ())), preferred_element_type=F32
        )

    def to_sibling(i, k):
        return remote(
            give.at[i, k], take.at[i, k], sib_send.at[i], sib_recv.at[i, k], sibling
        )

    def to_owner(i, w):
        used = pl.ds(0, 2 * own + 1)
        t = 2 * i + core
        return remote(
            spec_out.at[i, w, used], spec_in.at[t, chip, used],
            spec_send.at[i], spec_recv.at[t], places[w],
        )

    def to_others(make):
        for w in reversed(range(owners)):
            pl.when(me != places[w])(lambda: make(w).start())

    refs = pl.ds(0, 2 * own)

    def ref_to(w):
        return remote(ref_out.at[w], ref_in.at[me, refs], ref_send, ref_recv, places[w])

    span = width // pieces

    def row_chunk(z, c):
        out = jnp.dot(
            rowt[...], vol[z, :, c * CHUNK : (c + 1) * CHUNK], preferred_element_type=F32
        )
        out = out[:count] + out[count:]
        for b in range(CHUNK // LANES):
            here = slice(b * LANES, (b + 1) * LANES)
            begin = c * CHUNK + b * LANES
            rows[z, pad + begin : pad + begin + LANES, :] = out[:band, here].T
            extra[z, begin // LANES : begin // LANES + 1, :] = out[band : band + 1, here]

    def give_piece(k):
        for i in range(pairs):
            for b in range(span // LANES):
                here = slice(b * LANES, (b + 1) * LANES)
                give[i, k, here, :] = shifted(2 * i + 1 - core, k * span + b * LANES, LANES)
            to_sibling(i, k).start()

    def own_part(i):
        t = 2 * i + core
        for b in range(blocks):
            summed[b * LANES : (b + 1) * LANES, :] = shifted(t, b * LANES, LANES)

    def line_copy(i):
        return remote(line_give.at[i], line_take.at[i], line_send.at[i], line_recv.at[i], sibling)

    def last_line(i):
        line[...] = jnp.zeros(line.shape, F32)
        for k, t in enumerate((2 * i + core, 2 * i + 1 - core)):
            value = last_row(t)
            for b in range(blocks):
                line[k : k + 1, b * LANES : (b + 1) * LANES] = value[b : b + 1, :]
        value = line[...]
        high = value.astype(BF16).astype(F32)
        value = jnp.concatenate([high, value - high], axis=0).astype(BF16)
        one = along(value, colt[: 2 * band, :])
        two = along(value, colt[2 * band :, :])
        value = one[:SUBLANES] + one[SUBLANES:] + two[:SUBLANES]
        line_give[i] = jnp.zeros((SUBLANES, LANES), F32)
        for k in range(2 * band // LANES):
            here = slice(k * LANES, (k + 1) * LANES)
            line_keep[i, k : k + 1, :] = value[0:1, here]
            line_give[i, k : k + 1, :] = value[1:2, here]
        line_copy(i).start()

    each = span // LANES

    def near(i, b):
        here = slice(b * LANES, (b + 1) * LANES)
        if b % each == 0:
            to_sibling(i, b // each).wait_recv()
        begin = (b % each) * LANES
        total = summed[here, :] + take[i, b // each, begin : begin + LANES, :]
        summed[here, :] = total
        high, low = halves(total)
        stack[here, 0:LANES] = high
        stack[here, LANES : 2 * LANES] = low

    def far(b):
        here = slice(b * LANES, (b + 1) * LANES)
        high, low = halves(summed[b * LANES + 1 : (b + 1) * LANES + 1, :])
        stack[here, 2 * LANES : 3 * LANES] = high
        stack[here, 3 * LANES :] = low

    def merge(i, begin, end):
        for b in range(begin + (1 if begin else 0), min(end + 1, blocks)):
            near(i, b)
            if b > begin:
                far(b - 1)
        if end == blocks:
            far(blocks - 1)

    def put_line(i):
        line_copy(i).wait_recv()
        for w in range(owners):
            begin = w * 2 * own
            offset = begin % LANES
            k = begin // LANES
            block = line_keep[i, k : k + 1, :] + line_take[i, k : k + 1, :]
            if offset:
                block = pltpu.roll(jnp.broadcast_to(block, (SUBLANES, LANES)), LANES - offset, 1)
            spec_out[i, w, 2 * own : 2 * own + 1, :] = block[0:1]

    def gather(i, begin, end):
        deep = slice(begin * LANES, end * LANES)
        for c in range(chunks):
            here = slice(c * CHUNK, (c + 1) * CHUNK)
            picked = jnp.dot(onehot[i, here, deep], stack[deep, :], preferred_element_type=F32)
            near = picked[:, :LANES] + picked[:, LANES : 2 * LANES]
            far = picked[:, 2 * LANES : 3 * LANES] + picked[:, 3 * LANES :]
            part = shares[i, here, :]
            value = (1.0 - part) * near + part * far
            if begin:
                value = value + sofar[here, :]
            if end < blocks:
                sofar[here, :] = value
            else:
                high, low = halves(value)
                proj[here, :LANES] = high
                proj[here, LANES:] = low

    def columns(i):
        both = jnp.dot(colt[...], proj[...], preferred_element_type=F32)
        top = 2 * band
        value = both[:top, :LANES] + both[:top, LANES:] + both[top:, :LANES]
        for w in range(owners):
            spec_out[i, w, : 2 * own, :] = value[w * 2 * own : (w + 1) * 2 * own]

    get_table.wait()
    for copy in scalars:
        copy.wait()
    sent = 0
    for h in range(len(PARTS)):
        part = (slice(None), slice(None), columns_of(h))
        pltpu.make_async_copy(volume_ref.at[part], vol.at[part], sems.at[9 + h]).wait()
        for z in range(planes):
            for c in range(begins[h], ends[h]):
                row_chunk(z, c)
        if h == 0:
            wait_entry()
        known = ends[h] * CHUNK
        ready = pieces if known == width else (known - pad) // span
        for k in range(sent, ready):
            give_piece(k)
        sent = ready
    prepare_ref()
    to_others(ref_to)
    get_colt.wait()
    for i in range(pairs):
        last_line(i)
    for i in range(pairs):
        own_part(i)
        stops = [blocks * stop // 8 for stop in STOPS]
        for begin, end in zip([0] + stops[:-1], stops):
            merge(i, begin, end)
            gather(i, begin, end)
        columns(i)
        put_line(i)
        to_others(functools.partial(to_owner, i))

    def wave(ints):
        angle = (ints & (length - 1)).astype(F32) * (2.0 * math.pi / length)
        return jnp.cos(angle), jnp.sin(angle)

    def thirds(value, axis, order):
        high = value.astype(BF16)
        parts = (high, (value - high.astype(F32)).astype(BF16))
        return jnp.concatenate([parts[k] for k in order], axis=axis)

    slot = (me - first) // stride

    @pl.when(is_owner)
    def _():
        spot = lax.broadcasted_iota(jnp.int32, (n, band), 1)
        freq = jnp.where(spot < half, spot, jnp.where(spot == half, -half, half - spot))
        step = lax.broadcasted_iota(jnp.int32, (n, band), 0) - n // 2
        cols = lax.broadcasted_iota(jnp.int32, (own, win_cols), 0) + slot * own
        offset = lax.broadcasted_iota(jnp.int32, (own, win_cols), 1) - win_cols // 2
        row_waves, col_waves = [], []
        for t in range(tilts):
            cos, sin = wave(freq * (center_ref[t, 0] + step))
            row_waves.append(thirds(jnp.concatenate([cos, -sin], axis=1), 1, (0, 0, 1)))
            cos, sin = wave(cols * (center_ref[t, 1] + offset))
            col_waves.append(halves(jnp.concatenate([cos, -sin], axis=0)))
        spot = lax.broadcasted_iota(jnp.int32, (own, band), 1)
        lower, start, middle = spot < half, spot == 0, spot == half
        ref_in[me, refs] = ref_out[slot]
        arrived = ref_in.at[pl.ds(0, n - 1), refs]
        remote(arrived, arrived, ref_send, ref_recv, me).wait_recv()
        part_out[tilts * n :, :] = jnp.zeros((SUBLANES, win_cols), F32)

        def put_power(real, imag, row):
            power = jnp.sum(real * real + imag * imag, axis=0, keepdims=True)
            part_out[tilts * n + row : tilts * n + row + 1, :] = power

        owned = [ref_in[owner_ref[t], refs] for t in range(tilts)]
        for t in range(tilts):
            put_power(owned[t][:own], owned[t][own:], tilts + t)
        used = pl.ds(0, 2 * own + 1)
        for t in [*range(1, tilts, 2), *range(0, tilts, 2)]:
            remote_count = n // 2
            if t % 2 == 1:
                spec_in[t, chip, used] = spec_out[t // 2, slot, used]
                remote_count -= 1
            arrived = spec_in.at[t, pl.ds(0, remote_count), used]
            remote(arrived, arrived, spec_send.at[0], spec_recv.at[t], me).wait_recv()
            total = spec_in[t, 0, : 2 * own]
            last = spec_in[t, 0, 2 * own : 2 * own + 1]
            for e in range(1, n // 2):
                total = total + spec_in[t, e, : 2 * own]
                last = last + spec_in[t, e, 2 * own : 2 * own + 1]
            cos, sin = total[:own], total[own:]
            last = jnp.broadcast_to(last, (SUBLANES, band)).T[:, 0:1]
            last_cos, last_sin = last[:own], last[own : 2 * own]
            cos_turn = pltpu.roll(cos, half, 1)
            sin_turn = pltpu.roll(sin, half, 1)
            spec_re = jnp.where(
                lower,
                cos - jnp.where(start, 0.0, sin_turn),
                jnp.where(middle, cos + last_sin, cos_turn + sin),
            )
            spec_im = jnp.where(
                lower,
                -(jnp.where(start, 0.0, cos_turn) + sin),
                jnp.where(middle, last_cos - sin, cos - sin_turn),
            )
            ref_re, ref_im = owned[t][:own], owned[t][own:]
            cross_re = spec_re * ref_re + spec_im * ref_im
            cross_im = spec_im * ref_re - spec_re * ref_im
            put_power(spec_re, spec_im, t)
            cross = jnp.concatenate([
                jnp.concatenate([cross_re, cross_im], axis=1),
                jnp.concatenate([cross_im, -cross_re], axis=1),
            ], axis=0)
            high, low = halves(along(row_waves[t], thirds(cross, 1, (0, 1, 0))))
            near, far = col_waves[t]
            part_out[t * n : (t + 1) * n, :] = (
                jnp.dot(high, near, preferred_element_type=F32)
                + jnp.dot(high, far, preferred_element_type=F32)
                + jnp.dot(low, near, preferred_element_type=F32)
            )
        for d in range(n):
            @pl.when(me != d)
            def _():
                remote(part_out, part_in.at[slot], part_send, part_recv, d).start()
        part_in[slot] = part_out[...]

    def settle(ref, send, recv, sending):
        for fewer in range(2):
            @pl.when(is_owner == (fewer == 1))
            def _():
                part = ref.at[pl.ds(0, owners - fewer)]
                copy = remote(part, part, send, recv, me)
                if sending:
                    copy.wait_send()
                else:
                    copy.wait_recv()

    settle(part_in, part_send, part_recv, False)
    total = part_in[0]
    for w in range(1, owners):
        total = total + part_in[w]
    power = jnp.sum(total[tilts * n :], axis=1, keepdims=True) / (band * band) + 1e-06
    peaks = []
    mine_row = lax.broadcasted_iota(jnp.int32, (n, win_cols), 0) == me
    for t in range(tilts):
        scale = band * jnp.sqrt(power[t : t + 1] * power[tilts + t : tilts + t + 1])
        value = total[t * n : (t + 1) * n]
        row = jnp.sum(jnp.where(mine_row, value, 0.0), axis=0, keepdims=True)
        out_ref[t] = row / scale
        peaks.append(jnp.max(jnp.max(value, axis=0, keepdims=True), axis=1, keepdims=True) / scale)
    spot = lax.broadcasted_iota(jnp.int32, (1, win_cols), 1)
    best = jnp.broadcast_to(peaks[0], (1, win_cols))
    for t in range(1, tilts):
        best = jnp.where(spot == t, peaks[t], best)
    out_ref[tilts] = best

    settle(ref_out, ref_send, ref_recv, True)
    for i in range(pairs):
        remote(give.at[i], take.at[i], sib_send.at[i], sib_recv.at[i, 0], sibling).wait_send()
        line_copy(i).wait_send()
        settle(spec_out.at[i, :, pl.ds(0, 2 * own + 1)], spec_send.at[i], spec_recv.at[0], True)

    @pl.when(is_owner)
    def _():
        every = ref_in.at[pl.ds(0, n - 1), pl.ds(0, part_out.shape[0])]
        remote(every, every, part_send, part_recv, me).wait_send()


def finish_kernel(both_ref, corr_ref, peak_ref):
    tilts = corr_ref.shape[0]
    corr_ref[...] = both_ref[:tilts]
    peak_ref[...] = both_ref[tilts, 0, :tilts]


def run(n, volume, shift, weight, left, share, center, owner, mine):
    planes, height, width = volume.shape
    tilts = left.shape[0]
    pairs = tilts // 2
    band = mine.shape[-1]
    win_cols = band
    owners = OWNERS
    rowt = row_table(height, band)
    colt = col_table(width, band, owners)
    blocks = width // LANES
    pad = width // 16 + SUBLANES
    own = band // owners
    message = (2 * own + SUBLANES, band)
    part = (tilts * n + SUBLANES, win_cols)
    smem = pl.BlockSpec(memory_space=pltpu.SMEM)
    vmem = pl.BlockSpec(memory_space=pltpu.VMEM)
    hbm = pl.BlockSpec(memory_space=pl.ANY)
    dma = pltpu.SemaphoreType.DMA
    both = pl.pallas_call(
        functools.partial(fused_kernel, n, owners),
        out_shape=pltpu.VMEM((tilts + 1, 1, win_cols), F32),
        in_specs=[hbm] * 10,
        out_specs=vmem,
        scratch_shapes=[
            pltpu.SMEM(center.shape, jnp.int32),
            pltpu.SMEM(owner.shape, jnp.int32),
            pltpu.SMEM(shift.shape, jnp.int32),
            pltpu.SMEM(weight.shape, F32),
            pltpu.VMEM(left.shape, jnp.int32),
            pltpu.VMEM(share.shape, F32),
            pltpu.VMEM(mine.shape, F32),
            pltpu.VMEM((planes, height, width), BF16),
            pltpu.VMEM(rowt.shape, BF16),
            pltpu.VMEM(colt.shape, BF16),
            pltpu.VMEM((pairs, width, width), BF16),
            pltpu.VMEM((pairs, width, LANES), F32),
            pltpu.VMEM((planes, width + 2 * pad, LANES), F32),
            pltpu.VMEM((planes, blocks, LANES), F32),
            pltpu.VMEM((SUBLANES, width), F32),
            pltpu.VMEM((width + SUBLANES, LANES), F32),
            pltpu.VMEM((width, LANES), F32),
            pltpu.VMEM((pairs, PIECES, width // PIECES, LANES), F32),
            pltpu.VMEM((pairs, PIECES, width // PIECES, LANES), F32),
            pltpu.VMEM((width, 4 * LANES), BF16),
            pltpu.VMEM((width, 2 * LANES), BF16),
            pltpu.VMEM((band, band), F32),
            pltpu.VMEM((pairs, SUBLANES, LANES), F32),
            pltpu.VMEM((pairs, SUBLANES, LANES), F32),
            pltpu.VMEM((pairs, SUBLANES, LANES), F32),
            pltpu.VMEM((owners, 2 * own, band), F32),
            pltpu.VMEM((n, max(2 * own, part[0]), band), F32),
            pltpu.VMEM((pairs, owners) + message, F32),
            pltpu.VMEM((tilts, n // 2) + message, F32),
            pltpu.VMEM(part, F32),
            pltpu.VMEM((owners,) + part, F32),
            dma((9 + len(PARTS),)),
            dma, dma, dma((pairs,)), dma((pairs, PIECES)), dma((pairs,)), dma((pairs,)),
            dma((pairs,)), dma((tilts,)), dma, dma,
        ],
        compiler_params=pltpu.CompilerParams(
            collective_id=0, has_side_effects=True, vmem_limit_bytes=56 * 1024 * 1024
        ),
        name="fused",
    )(
        center, owner, shift, weight, left, share, mine,
        volume, jnp.asarray(rowt), jnp.asarray(colt),
    )
    both = pltpu.with_memory_space_constraint(both, pltpu.VMEM)
    return pl.pallas_call(
        finish_kernel,
        out_shape=(
            jax.ShapeDtypeStruct((tilts, 1, win_cols), F32),
            jax.ShapeDtypeStruct((tilts,), F32),
        ),
        in_specs=[vmem],
        out_specs=(vmem, vmem),
        name="finish",
    )(both)


def solution(mesh):
    n = mesh.shape["slab"]

    def per_device(volume, shift, weight, left, share, center, owner, bands):
        return run(n, volume, shift, weight, left, share, center, owner, bands)

    placed = (
        P(("grp", "slab"), None, None),
        P("grp", "slab"),
        P("grp", "slab"),
        P("grp", None),
        P("grp", None),
        P("grp", None),
        P("grp"),
        P(("grp", "slab"), None, None, None),
    )
    return jax.shard_map(
        per_device,
        mesh=mesh,
        in_specs=placed,
        out_specs=(P("grp", "slab", None), P("grp")),
        check_vma=False,
    )
```
